128 devices in a mesh: field: 2 (over core), dom: 64 (over x, y, z).
Axes of the slice: x: 4, y: 4, z: 4, core: 2. Of those that a mesh axis runs over, the one named last changes fastest.
Arguments:
- modes: float32 [2, 40, 524288], P('field', None, 'dom'), may hold values from -6 to 6
- previous: float32 [2, 40, 524288], P('field', None, 'dom'), may hold values from -6 to 6
- kinds: int32 [2, 3, 1024], P('field'), may hold values from 0 to 3
- scales: float32 [2, 3, 1024], P('field'), may hold values from 0.5 to 4
- tables: bfloat16 [2, 3, 4, 512, 512], P('field'), may hold values from -2 to 6, as said below
- wet_rows: int32 [2, 196608], P('field', 'dom'), may hold values from 0 to 8191, as said below
- wet_counts: int32 [64], P('dom'), may hold values from 768 to 3072, as said below
- coupling: float32 [196608], P('dom'), may hold values from -6 to 6
Outputs:
- basis: float32 [2, 120, 524288], P('field', None, 'dom')
- projected: float32 [120, 120], replicated
The draws below stay inside these ranges and needn't reach their ends.
Inputs may be any that keep to these rules, and one draw needn't show every extreme that they name: `tables`: tables of offset 0 are symmetric. `wet_rows`: within each subdomain and field the 3072 row numbers are distinct. `wet_counts`: some subdomain uses all 3072 slots.
All inputs are finite; a program needn't handle non-finite values.
Results may differ from the reference program's by a relative error of at most 0.00045.
The reference program's roundings to bfloat16 on the way count: a program that leaves them out, or rounds other values in their place, can miss the bound.
Values may be sent and summed in bfloat16 or wider, within the bound.
No kernel may reach another device: no remote copies, remote signals or barrier semaphores. Data moves between devices by JAX's collectives and lax.ppermute only.
A program may use at most 192 MiB of HBM per device.

```python
import math
import jax
import jax.numpy as jnp
from jax import lax

MODES = 40
BS = 512
NTYPE = 4
NBR = 16
ROWS_DEV = 8192
IFACE = 3072
SUBDOMS = 64
NBLK = 1024
NF = 524288


def draw_tables(key, part):
    first, second = jax.random.split(key, 2)
    shape = (2, 3, NTYPE, BS, BS)
    noise = jnp.clip(jax.random.normal(first, shape, jnp.float32), -4.0, 4.0)
    noise = noise / jnp.sqrt(jnp.float32(BS))
    symmetric = (noise + jnp.swapaxes(noise, -1, -2)) * 0.70710678
    diagonal = jax.random.uniform(second, (2, 3, NTYPE, BS), jnp.float32, 2.0, 4.0)
    identity = jnp.eye(BS, dtype=jnp.float32)
    centre = symmetric + identity * diagonal[..., None]
    which = jnp.arange(3)[None, :, None, None, None] == 0
    return jnp.where(which, centre, noise).astype(jnp.bfloat16)


def draw_wet_rows(key, part):
    keys = jax.random.split(jax.random.fold_in(key, 11), 2 * SUBDOMS)
    chosen = jax.vmap(lambda single: jax.random.permutation(single, ROWS_DEV)[:IFACE])(keys)
    return chosen.reshape(2, SUBDOMS * IFACE).astype(jnp.int32)


def draw_wet_counts(key, part):
    first, second = jax.random.split(jax.random.fold_in(key, 23), 2)
    counts = jax.random.randint(first, (SUBDOMS,), IFACE // 4, IFACE + 1)
    fullest = jax.random.randint(second, (), 0, SUBDOMS)
    return jnp.where(jnp.arange(SUBDOMS) == fullest, IFACE, counts).astype(jnp.int32)


def place_ends(array, own_key, smallest, high):
    longest = array.shape.index(max(array.shape))
    spots = []
    for shift in (0, 1):
        where = [jax.random.randint(jax.random.fold_in(own_key, axis), (), 0, length) for axis, length in enumerate(array.shape)]
        where[longest] = (where[longest] + shift) % array.shape[longest]
        spots.append(tuple(where))
    return array.at[spots[0]].set(smallest).at[spots[1]].set(high)


def block_scale(own_key, extent, cuts, smallest, top_value):
    def one(position, parts):
        heights = jax.random.uniform(jax.random.fold_in(jax.random.fold_in(own_key, 6), position), (parts,), jnp.float32, smallest / len(cuts), top_value / len(cuts))
        return jnp.repeat(jnp.exp(heights), extent[position] // parts).reshape((-1,) + (1,) * (len(extent) - position - 1))

    factor_of = one(*cuts[0])
    for cut in cuts[1:]:
        factor_of = factor_of * one(*cut)
    return factor_of


def bell_draw(own_key, shape, deviation, limit, cuts=(), kind=jnp.bfloat16):
    values = jax.random.normal(own_key, shape, jnp.float32) * deviation
    if len(cuts) > 0:
        values = block_scale(own_key, shape, cuts, -0.22, 0.18) * values
    return jnp.clip(values, min=-limit, max=limit).astype(kind)


def setup_inputs(seed: int = 0) -> dict:
    splits = jax.random.split(jax.random.key(seed), 9)
    return {
        "modes": bell_draw(splits[0], (2, MODES, NF), 1.0, 6.0, ((0, 2), (2, 64)), jnp.float32),
        "previous": bell_draw(splits[1], (2, MODES, NF), 1.0, 6.0, ((0, 2), (2, 64)), jnp.float32),
        "kinds": place_ends(jax.random.randint(splits[2], (2, 3, NBLK), 0, NTYPE), jax.random.fold_in(splits[2], 1), 0, NTYPE - 1).astype(jnp.int32),
        "scales": jnp.clip(jnp.exp(math.log(4.0) - 2.0794415 * jax.random.uniform(splits[3], (2, 3, NBLK), jnp.float32) ** block_scale(splits[3], (2, 3, NBLK), ((0, 2),), -0.2, 0.2)), 0.5, 4.0),
        "tables": draw_tables(jax.random.fold_in(splits[8], 71), 0),
        "wet_rows": draw_wet_rows(jax.random.fold_in(splits[8], 71), 0),
        "wet_counts": draw_wet_counts(jax.random.fold_in(splits[8], 71), 0),
        "coupling": bell_draw(splits[7], (SUBDOMS * IFACE,), 1.0, 6.0, ((0, 64),), jnp.float32),
    }


def block_product(window, kinds, scales, tables):
    columns = window.shape[0]
    blocks = window.reshape(columns, NBR + 4, BS).astype(jnp.float32)
    centre = tables[0][kinds[0, 2:]].astype(jnp.float32)
    result = scales[0, 2:][None, :, None] * jnp.einsum('cni,nji->cnj', blocks[:, 2:NBR + 2], centre)
    for offset in (1, 2):
        ahead = tables[offset][kinds[offset, 2:]].astype(jnp.float32)
        result = result + scales[offset, 2:][None, :, None] * jnp.einsum('cni,nji->cnj', blocks[:, 2 + offset:NBR + 2 + offset], ahead)
        behind = tables[offset][kinds[offset, 2 - offset:NBR + 2 - offset]].astype(jnp.float32)
        result = result + scales[offset, 2 - offset:NBR + 2 - offset][None, :, None] * jnp.einsum('cni,nij->cnj', blocks[:, 2 - offset:NBR + 2 - offset], behind)
    return result.reshape(columns, NBR * BS)

def field_blocks(vectors, kinds, scales, tables):
    columns = vectors.shape[0]
    padded = jnp.pad(vectors.astype(jnp.bfloat16), ((0, 0), (2 * BS, 2 * BS)))
    kinds_pad = jnp.pad(kinds, ((0, 0), (2, 0)))
    scales_pad = jnp.pad(scales, ((0, 0), (2, 0)))

    def one_domain(domain):
        window = lax.dynamic_slice_in_dim(padded, domain * ROWS_DEV, ROWS_DEV + 4 * BS, 1)
        local_kinds = lax.dynamic_slice_in_dim(kinds_pad, domain * NBR, NBR + 2, 1)
        local_scales = lax.dynamic_slice_in_dim(scales_pad, domain * NBR, NBR + 2, 1)
        return block_product(window, local_kinds, local_scales, tables)
    pieces = lax.map(one_domain, jnp.arange(SUBDOMS, dtype=jnp.int32))
    return jnp.transpose(pieces, (1, 0, 2)).reshape(columns, SUBDOMS * ROWS_DEV)

def operator(vectors, kinds, scales, tables, global_rows, weights):
    images = [field_blocks(vectors[field_id], kinds[field_id], scales[field_id], tables[field_id]) for field_id in range(2)]
    coupled = []
    for field_id in range(2):
        other = 1 - field_id
        values = vectors[other][:, global_rows[other]] * weights[None, :]
        coupled.append(images[field_id].at[:, global_rows[field_id]].add(values))
    return jnp.stack(coupled)

def reference(modes, previous, kinds, scales, tables, wet_rows, wet_counts, coupling):
    highest = lax.Precision.HIGHEST
    offsets = jnp.arange(SUBDOMS, dtype=jnp.int32)[:, None] * ROWS_DEV
    global_rows = (wet_rows.reshape(2, SUBDOMS, IFACE) + offsets[None]).reshape(2, SUBDOMS * IFACE)
    used = jnp.arange(IFACE, dtype=jnp.int32)[None, :] < wet_counts[:, None]
    weights = jnp.where(used, coupling.reshape(SUBDOMS, IFACE), jnp.float32(0.0)).reshape(SUBDOMS * IFACE)
    image_x = operator(modes, kinds, scales, tables, global_rows, weights)
    quotient = jnp.sum(modes * image_x, axis=(0, 2)) / jnp.sum(modes * modes, axis=(0, 2))
    diag_table = jnp.diagonal(tables[:, 0], axis1=-2, axis2=-1).astype(jnp.float32)
    jacobi = jnp.stack([(scales[field_id, 0][:, None] * diag_table[field_id][kinds[field_id, 0]]).reshape(SUBDOMS * ROWS_DEV) for field_id in range(2)])
    residual_dir = (image_x - modes * quotient[None, :, None]) / jacobi[:, None, :]
    image_wp = operator(jnp.concatenate([residual_dir, previous], axis=1), kinds, scales, tables, global_rows, weights)
    search = jnp.concatenate([modes, residual_dir, previous], axis=1)
    image_all = jnp.concatenate([image_x, image_wp], axis=1)
    ndof = 2.0 * SUBDOMS * ROWS_DEV
    gram_b = (jnp.dot(search[0], search[0].T, precision=highest) + jnp.dot(search[1], search[1].T, precision=highest)) / ndof
    raw = jnp.dot(search[0], image_all[0].T, precision=highest) + jnp.dot(search[1], image_all[1].T, precision=highest)
    gram_a = (raw + raw.T) / (2.0 * ndof)
    chol = jnp.linalg.cholesky(gram_b)
    leading = jax.scipy.linalg.solve_triangular(chol, gram_a, lower=True)
    projected = jax.scipy.linalg.solve_triangular(chol, leading.T, lower=True)
    basis = jnp.stack([jax.scipy.linalg.solve_triangular(chol, search[field_id], lower=True) for field_id in range(2)])
    return (basis, projected)
```

```python
import functools

import jax
import jax.numpy as jnp
from jax import lax
from jax.experimental import pallas as pl
from jax.experimental.pallas import tpu as pltpu
from jax.sharding import Mesh
from jax.sharding import PartitionSpec as P

BS = 512
NTYPE = 4
NBR = 16
ROWS = NBR * BS
HALO = 2 * BS
MODES = 40
IFACE = 3072
LANES = 128
TILES = ROWS // LANES
DOM = ("dom_0", "dom_1", "dom_2")
FIELD_DOM = ("field", "dom_0", "dom_1", "dom_2")
ALL_DEV = 128
F32 = jnp.float32
BF16 = jnp.bfloat16

VMEM = pl.BlockSpec(memory_space=pltpu.VMEM)
SMEM = pl.BlockSpec(memory_space=pltpu.SMEM)
ANY = pl.BlockSpec(memory_space=pl.ANY)

OPS = (
    (0, 0, True, 160),
    (1, -1, True, 160),
    (2, -2, True, 160),
    (1, 1, False, 160),
    (2, 2, False, 128),
)


def params(mib):
    return pltpu.CompilerParams(vmem_limit_bytes=mib << 20)


def shape(*dims, kind=F32):
    return jax.ShapeDtypeStruct(dims, kind)


def domain_index():
    return (lax.axis_index(DOM[0]) * 4 + lax.axis_index(DOM[1])) * 4 + lax.axis_index(DOM[2])


def swap_field(value):
    return lax.ppermute(value, "field", [(0, 1), (1, 0)])


def from_left(value):
    return lax.ppermute(value, DOM, [(i, i + 1) for i in range(63)])


def from_right(value):
    return lax.ppermute(value, DOM, [(i + 1, i) for i in range(63)])


def exchange(rows):
    return lax.all_to_all(rows, FIELD_DOM, 0, 0, tiled=True)


def round_kernel(modes, prev, modes_b, modes_h, modes_t, prev_b, prev_h, prev_t):
    for source, whole, head, tail in (
        (modes, modes_b, modes_h, modes_t),
        (prev, prev_b, prev_h, prev_t),
    ):
        rounded = source[...].astype(BF16)
        whole[...] = rounded
        head[...] = rounded[:, :HALO]
        tail[...] = rounded[:, ROWS - HALO :]


def rounded_parts(modes, prev):
    whole = shape(MODES, ROWS, kind=BF16)
    end = shape(MODES, HALO, kind=BF16)
    return pl.pallas_call(
        round_kernel,
        out_shape=(whole, end, end) * 2,
        in_specs=[VMEM] * 2,
        out_specs=[VMEM] * 6,
        compiler_params=params(24),
        name="rounded",
    )(modes, prev)


def apply_operator(
    vec, left, right, other, tables, kinds, scales, rows, rows_o, weights,
    copies, blocks, even, odd, acc, tab, other_t, coup, product,
):
    for copy in copies:
        copy.start()
    for b in range(2):
        blocks[b * MODES : (b + 1) * MODES, :] = left[:, b * BS : (b + 1) * BS].astype(F32)
        at = (NBR + 2 + b) * MODES
        blocks[at : at + MODES, :] = right[:, b * BS : (b + 1) * BS].astype(F32)
    for b in range(NBR):
        at = (b + 2) * MODES
        blocks[at : at + MODES, :] = vec[:, b * BS : (b + 1) * BS]
    even[...] = blocks[...].astype(BF16)
    odd[...] = blocks[MODES : (NBR + 3) * MODES, :].astype(BF16)
    for c in range(TILES):
        piece = other[:, c * LANES : (c + 1) * LANES].astype(F32)
        other_t[c * LANES : (c + 1) * LANES, :MODES] = piece.T
    coup[...] = jnp.zeros_like(coup)
    acc[...] = jnp.zeros_like(acc)
    first = domain_index() * NBR
    done = 0
    for index, (offset, shift, transposed, slots) in enumerate(OPS):
        if index < 3:
            copies[index].wait()
        source, at = (odd, (1 + shift) * MODES) if shift % 2 else (even, (2 + shift) * MODES)
        kshift = shift if transposed else 0

        def step(kind, carry, offset=offset, source=source, at=at, kshift=kshift,
                 transposed=transposed, slots=slots, done=done):
            product[...] = lax.dot_general(
                source[at : at + NBR * MODES, :],
                tab[offset * NTYPE + kind],
                (((1,), (0 if transposed else 1,)), ((), ())),
                preferred_element_type=F32,
            )
            base = done + kind * slots
            for u in range(slots):
                slot = base + u
                coup[pl.ds(rows[slot], 1), :] = other_t[pl.ds(rows_o[slot], 1), :] * weights[slot]
            for b in range(NBR):
                block = jnp.maximum(first + b + kshift, 0)
                factor = jnp.where(
                    kinds[offset, block] == kind, scales[offset, block], jnp.float32(0.0)
                )
                span = slice(b * MODES, (b + 1) * MODES)
                acc[span, :] += factor * product[span, :]
            return carry

        lax.fori_loop(0, NTYPE, step, 0)
        done += NTYPE * slots


def image_tile(acc, coup, c):
    b, part = divmod(c, BS // LANES)
    blocked = acc[b * MODES : (b + 1) * MODES, part * LANES : (part + 1) * LANES]
    return blocked + coup[c * LANES : (c + 1) * LANES, :].T[:MODES, :]


def stage_scratch():
    return [
        pltpu.SemaphoreType.DMA((3,)),
        pltpu.VMEM(((NBR + 4) * MODES, BS), F32),
        pltpu.VMEM(((NBR + 4) * MODES, BS), BF16),
        pltpu.VMEM(((NBR + 2) * MODES, BS), BF16),
        pltpu.VMEM((NBR * MODES, BS), F32),
        pltpu.VMEM((3 * NTYPE, BS, BS), BF16),
        pltpu.VMEM((ROWS, LANES), F32),
        pltpu.VMEM((ROWS, LANES), F32),
        pltpu.VMEM((NBR * MODES, BS), F32),
    ]


def table_copies(tables, tab, sems):
    return [
        pltpu.make_async_copy(
            tables.at[pl.ds(k * NTYPE, NTYPE)], tab.at[pl.ds(k * NTYPE, NTYPE)], sems.at[k]
        )
        for k in range(3)
    ]


def modes_kernel(
    vec, left, right, other, tables, kinds, scales, rows, rows_o, weights,
    image, jacobi, sums, sems, blocks, even, odd, acc, tab, other_t, coup, product,
):
    apply_operator(
        vec, left, right, other, tables, kinds, scales, rows, rows_o, weights,
        table_copies(tables, tab, sems), blocks, even, odd, acc, tab, other_t, coup, product,
    )
    squares = jnp.zeros((MODES, LANES), F32)
    products = jnp.zeros((MODES, LANES), F32)
    for c in range(TILES):
        span = slice(c * LANES, (c + 1) * LANES)
        value = image_tile(acc, coup, c)
        image[:, span] = value
        own = vec[:, span]
        squares += own * own
        products += own * value
    both = jnp.concatenate([squares, products, jnp.zeros((LANES - 2 * MODES, LANES), F32)], axis=0)
    total = jnp.sum(both.T, axis=0, keepdims=True)
    sums[...] = jnp.broadcast_to(total, (ALL_DEV, LANES))
    first = domain_index() * NBR
    on_diagonal = lax.broadcasted_iota(jnp.int32, (LANES, LANES), 0) == lax.broadcasted_iota(
        jnp.int32, (LANES, LANES), 1
    )
    for part in range(BS // LANES):
        span = slice(part * LANES, (part + 1) * LANES)
        lines = [
            jnp.sum(
                jnp.where(on_diagonal, tab[kind, span, span].astype(F32), 0.0), axis=0, keepdims=True
            )
            for kind in range(NTYPE)
        ]
        for b in range(NBR):
            kind = kinds[0, first + b]
            line = lines[0]
            for other_kind in range(1, NTYPE):
                line = jnp.where(kind == other_kind, lines[other_kind], line)
            at = b * BS + part * LANES
            jacobi[:, at : at + LANES] = scales[0, first + b] * line


def previous_kernel(
    vec, left, right, other, tables, kinds, scales, rows, rows_o, weights,
    image, sems, blocks, even, odd, acc, tab, other_t, coup, product,
):
    apply_operator(
        vec, left, right, other, tables, kinds, scales, rows, rows_o, weights,
        table_copies(tables, tab, sems), blocks, even, odd, acc, tab, other_t, coup, product,
    )
    for c in range(TILES):
        image[:, c * LANES : (c + 1) * LANES] = image_tile(acc, coup, c)


def stage_specs():
    return [VMEM, VMEM, VMEM, VMEM, ANY, SMEM, SMEM, SMEM, SMEM, SMEM]


def residual_kernel(gathered, modes, image, jacobi, residual, rounded, head, tail):
    total = jnp.sum(gathered[...], axis=0, keepdims=True)
    column = jnp.broadcast_to(total, (LANES, LANES)).T
    quotient = column[MODES : 2 * MODES, :] / column[:MODES, :]
    for c in range(TILES):
        span = slice(c * LANES, (c + 1) * LANES)
        value = (image[:, span] - modes[:, span] * quotient) / jacobi[:, span]
        residual[:, span] = value
        low = value.astype(BF16)
        rounded[:, span] = low
        if c < HALO // LANES:
            head[:, span] = low
        if c >= TILES - HALO // LANES:
            at = (c - (TILES - HALO // LANES)) * LANES
            tail[:, at : at + LANES] = low


def gram_kernel(
    vec, left, right, other, tables, kinds, scales, rows, rows_o, weights,
    modes, prev, image_x, image_p, packed,
    sems, blocks, even, odd, acc, tab, other_t, coup, product, image_r, gram,
):
    apply_operator(
        vec, left, right, other, tables, kinds, scales, rows, rows_o, weights,
        table_copies(tables, tab, sems), blocks, even, odd, acc, tab, other_t, coup, product,
    )
    for c in range(TILES):
        image_r[:, c * LANES : (c + 1) * LANES] = image_tile(acc, coup, c)
    gram[...] = jnp.zeros_like(gram)

    def step(b, carry):
        span = pl.ds(pl.multiple_of(b * BS, BS), BS)
        both = jnp.concatenate(
            [ref[:, span] for ref in (modes, vec, prev, image_x, image_r, image_p)], axis=0
        )
        high = both.astype(BF16)
        low = (both - high.astype(F32)).astype(BF16)
        gram[...] += lax.dot_general(
            jnp.concatenate([high, low], axis=0), high, (((1,), (1,)), ((), ())),
            preferred_element_type=F32,
        )
        return carry

    lax.fori_loop(0, NBR, step, 0)
    n = 3 * MODES
    pad = LANES - n
    zero_r = jnp.zeros((pad, n), F32)
    zero_c = jnp.zeros((LANES, pad), F32)

    def square(top, lane):
        value = gram[top : top + n, lane : lane + n]
        return jnp.concatenate([jnp.concatenate([value, zero_r], axis=0), zero_c], axis=1)

    cross_b = square(2 * n, 0)
    gram_b = square(0, 0) + cross_b + cross_b.T
    cross_a = square(0, n) + square(2 * n, n)
    raw = cross_a + square(3 * n, 0).T
    gram_a = raw + raw.T
    row = lax.broadcasted_iota(jnp.int32, (LANES, LANES), 0)
    col = lax.broadcasted_iota(jnp.int32, (LANES, LANES), 1)
    diagonal = jnp.sum(jnp.where(row == col, gram_a, 0.0), axis=0, keepdims=True)
    merged = jnp.where(row >= col, gram_b, gram_a)
    packed[...] = jnp.where(row == n, jnp.broadcast_to(diagonal, (LANES, LANES)), merged)


def final_kernel(packed, modes, residual, prev, basis, projected, inverse):
    n = 3 * MODES

    @pl.when(pl.program_id(0) == 0)
    def _():
        row = lax.broadcasted_iota(jnp.int32, (LANES, LANES), 0)
        col = lax.broadcasted_iota(jnp.int32, (LANES, LANES), 1)
        merged = packed[...]
        flipped = merged.T
        inside = (row < n) & (col < n)
        ndof = jnp.float32(2.0 * 64 * ROWS)
        gram_b = jnp.where(row >= col, merged, flipped) / ndof
        gram_b = jnp.where(inside, gram_b, jnp.where(row == col, 1.0, 0.0))
        diagonal = jnp.broadcast_to(merged[n : n + 1, :], (LANES, LANES))
        gram_a = jnp.where(row < col, merged, flipped)
        gram_a = jnp.where(row == col, diagonal, gram_a) / (2.0 * ndof)
        gram_a = jnp.where(inside, gram_a, 0.0)
        left = gram_b
        right = jnp.where(row == col, 1.0, 0.0).astype(F32)
        for j in range(n):
            pivot = jnp.broadcast_to(left[:, j : j + 1], (LANES, LANES))
            line_l = left[j : j + 1, :]
            line_r = right[j : j + 1, :]
            root = lax.rsqrt(pivot[j : j + 1, :])
            line_l = line_l * root
            line_r = line_r * root
            factor = jnp.where(row > j, pivot * root, 0.0)
            keep = row == j
            left = jnp.where(keep, line_l, left - factor * line_l)
            right = jnp.where(keep, line_r, right - factor * line_r)
        right = jnp.where(inside, right, 0.0)
        half = lax.dot_general(
            right, gram_a, (((1,), (0,)), ((), ())),
            precision=lax.Precision.HIGHEST, preferred_element_type=F32,
        )
        whole = lax.dot_general(
            half, right, (((1,), (1,)), ((), ())),
            precision=lax.Precision.HIGHEST, preferred_element_type=F32,
        )
        projected[...] = whole[:n, :n]
        inverse[...] = right

    factors = inverse[...][:n, :n]
    high = factors.astype(BF16)
    low = (factors - high.astype(F32)).astype(BF16)
    search = jnp.concatenate([modes[...], residual[...], prev[...]], axis=0)
    search_h = search.astype(BF16)
    search_l = (search - search_h.astype(F32)).astype(BF16)
    top = jnp.concatenate([high, high], axis=1)
    stacked = jnp.concatenate([search_h, search_l], axis=0)
    dims = (((1,), (0,)), ((), ()))
    basis[...] = lax.dot_general(top, stacked, dims, preferred_element_type=F32) + lax.dot_general(
        low, search_h, dims, preferred_element_type=F32
    )


def shards(modes, previous, kinds, scales, tables, wet_rows, wet_counts, coupling):
    modes = modes[0]
    prev = previous[0]
    kinds = kinds[0]
    scales = scales[0]
    tables = tables[0].reshape(3 * NTYPE, BS, BS)
    rows = wet_rows[0]
    used = jnp.arange(IFACE, dtype=jnp.int32) < wet_counts[0]
    weights = jnp.where(used, coupling, jnp.float32(0.0))
    rows_o = swap_field(rows)
    modes_b, modes_h, modes_t, prev_b, prev_h, prev_t = rounded_parts(modes, prev)
    rest = (tables, kinds, scales, rows, rows_o, weights)
    plane = shape(MODES, ROWS)
    image_x, jacobi, sums = pl.pallas_call(
        modes_kernel,
        out_shape=(plane, shape(1, ROWS), shape(ALL_DEV, LANES)),
        in_specs=stage_specs(),
        out_specs=[VMEM] * 3,
        scratch_shapes=stage_scratch(),
        compiler_params=params(48),
        name="modes",
    )(modes, from_left(modes_t), from_right(modes_h), swap_field(modes_b), *rest)
    gathered = exchange(sums)
    image_p = pl.pallas_call(
        previous_kernel,
        out_shape=plane,
        in_specs=stage_specs(),
        out_specs=VMEM,
        scratch_shapes=stage_scratch(),
        compiler_params=params(48),
        name="previous",
    )(prev, from_left(prev_t), from_right(prev_h), swap_field(prev_b), *rest)
    end = shape(MODES, HALO, kind=BF16)
    residual, residual_b, residual_h, residual_t = pl.pallas_call(
        residual_kernel,
        out_shape=(plane, shape(MODES, ROWS, kind=BF16), end, end),
        in_specs=[VMEM] * 4,
        out_specs=[VMEM] * 4,
        compiler_params=params(24),
        name="residual",
    )(gathered, modes, image_x, jacobi)
    packed = pl.pallas_call(
        gram_kernel,
        out_shape=shape(LANES, LANES),
        in_specs=stage_specs() + [VMEM] * 4,
        out_specs=VMEM,
        scratch_shapes=stage_scratch()
        + [pltpu.VMEM((MODES, ROWS), F32), pltpu.VMEM((12 * MODES, 6 * MODES), F32)],
        compiler_params=params(56),
        name="gram",
    )(
        residual, from_left(residual_t), from_right(residual_h), swap_field(residual_b), *rest,
        modes, prev, image_x, image_p,
    )
    part = jnp.sum(exchange(packed), axis=0, keepdims=True)
    packed = exchange(jnp.broadcast_to(part, (ALL_DEV, LANES)))
    width = 1024
    piece = pl.BlockSpec((MODES, width), lambda i: (0, i))
    n = 3 * MODES
    basis, projected = pl.pallas_call(
        final_kernel,
        out_shape=(shape(n, ROWS), shape(n, n)),
        grid=(ROWS // width,),
        in_specs=[pl.BlockSpec((LANES, LANES), lambda i: (0, 0)), piece, piece, piece],
        out_specs=[
            pl.BlockSpec((n, width), lambda i: (0, i)),
            pl.BlockSpec((n, n), lambda i: (0, 0)),
        ],
        scratch_shapes=[pltpu.VMEM((LANES, LANES), F32)],
        compiler_params=params(24),
        name="final",
    )(packed, modes, residual, prev)
    return (basis[None], projected)


def solution(mesh):
    finer = Mesh(
        mesh.devices.reshape(mesh.shape["field"], 4, 4, 4), ("field", "dom_0", "dom_1", "dom_2")
    )
    placed = (
        P("field", None, DOM),
        P("field", None, DOM),
        P("field", None, None),
        P("field", None, None),
        P("field", None, None, None, None),
        P("field", DOM),
        P(DOM),
        P(DOM),
    )
    return jax.shard_map(
        shards, mesh=finer, in_specs=placed, out_specs=(P("field", None, DOM), P()), check_vma=False
    )
```

```python
import functools

import jax
import jax.numpy as jnp
from jax import lax
from jax.experimental import pallas as pl
from jax.experimental.pallas import tpu as pltpu
from jax.sharding import Mesh
from jax.sharding import PartitionSpec as P

BS = 512
NTYPE = 4
NBR = 16
ROWS = NBR * BS
HALO = 2 * BS
MODES = 40
IFACE = 3072
LANES = 128
TILES = ROWS // LANES
DOM = ("dom_0", "dom_1", "dom_2")
FIELD_DOM = ("field", "dom_0", "dom_1", "dom_2")
ALL_DEV = 128
F32 = jnp.float32
BF16 = jnp.bfloat16

VMEM = pl.BlockSpec(memory_space=pltpu.VMEM)
SMEM = pl.BlockSpec(memory_space=pltpu.SMEM)
PAIR = 2 * MODES
SINGLE = 48
UNROLL = 2
SLOTS = IFACE // NBR

OPS = ((0, 0, 0, 0), (1, -1, -1, 0), (2, -2, -2, 0), (1, 1, 0, 1), (2, 2, 0, 1))


def params(mib):
    return pltpu.CompilerParams(vmem_limit_bytes=mib << 20)


def shape(*dims, kind=F32):
    return jax.ShapeDtypeStruct(dims, kind)


def domain_index():
    return (lax.axis_index(DOM[0]) * 4 + lax.axis_index(DOM[1])) * 4 + lax.axis_index(DOM[2])


def swap_field(value):
    return lax.ppermute(value, "field", [(0, 1), (1, 0)])


def from_left(value):
    return lax.ppermute(value, DOM, [(i, i + 1) for i in range(63)])


def from_right(value):
    return lax.ppermute(value, DOM, [(i + 1, i) for i in range(63)])


def exchange(rows):
    return lax.all_to_all(rows, FIELD_DOM, 0, 0, tiled=True)


def round_kernel(modes, prev, whole, head, tail):
    rounded = jnp.concatenate([modes[...], prev[...]], axis=0).astype(BF16)
    whole[...] = rounded
    head[...] = rounded[:, :HALO]
    tail[...] = rounded[:, ROWS - HALO :]


def rounded_parts(modes, prev):
    end = shape(PAIR, HALO, kind=BF16)
    return pl.pallas_call(
        round_kernel,
        out_shape=(shape(PAIR, ROWS, kind=BF16), end, end),
        in_specs=[VMEM] * 2,
        out_specs=[VMEM] * 3,
        compiler_params=params(24),
        name="rounded",
    )(modes, prev)


def products(blocks, tables, flipped, kinds, scales, rows, rows_o, weights, other_t, coup, put):
    first = domain_index() * NBR

    def step(index, carry):
        for u in range(UNROLL):
            b = index * UNROLL + u
            total = None
            for offset, shift, owner, flip in OPS:
                block = jnp.maximum(first + b + owner, 0)
                kind = kinds[offset, block]
                if flip:
                    table = flipped[(offset - 1) * NTYPE + kind]
                else:
                    table = tables[offset * NTYPE + kind]
                product = jnp.dot(blocks[b + 2 + shift], table, preferred_element_type=F32)
                product = scales[offset, block] * product
                total = product if total is None else total + product
            put(pl.ds(pl.multiple_of(b * BS, BS), BS), total)
            for v in range(SLOTS):
                slot = b * SLOTS + v
                coup[pl.ds(rows[slot], 1), :] = other_t[pl.ds(rows_o[slot], 1), :] * weights[slot]
        return carry

    lax.fori_loop(0, NBR // UNROLL, step, 0)


def first_kernel(
    modes, prev, left, right, other, tables, kinds, scales, rows, rows_o, weights,
    image_x, image_p, ratios, head, tail, sums, flipped,
    blocks, other_t, coup,
):
    for index in range(2 * NTYPE):
        flipped[index] = tables[NTYPE + index].T
    for b in range(2):
        span = slice(b * BS, (b + 1) * BS)
        blocks[b] = left[:, span]
        blocks[NBR + 2 + b] = right[:, span]
    for b in range(NBR):
        span = slice(b * BS, (b + 1) * BS)
        blocks[b + 2] = jnp.concatenate([modes[:, span], prev[:, span]], axis=0).astype(BF16)
    for c in range(TILES):
        span = slice(c * LANES, (c + 1) * LANES)
        other_t[span, :PAIR] = other[:, span].astype(F32).T
    coup[...] = jnp.zeros_like(coup)

    def put(span, total):
        image_x[:, span] = total[:MODES]
        image_p[:, span] = total[MODES:]

    products(blocks, tables, flipped, kinds, scales, rows, rows_o, weights, other_t, coup, put)
    first = domain_index() * NBR
    on_diagonal = lax.broadcasted_iota(jnp.int32, (LANES, LANES), 0) == lax.broadcasted_iota(
        jnp.int32, (LANES, LANES), 1
    )
    lines = []
    for part in range(BS // LANES):
        span = slice(part * LANES, (part + 1) * LANES)
        lines.append(
            [
                jnp.sum(
                    jnp.where(on_diagonal, tables[kind, span, span].astype(F32), 0.0),
                    axis=0, keepdims=True,
                )
                for kind in range(NTYPE)
            ]
        )
    squares = jnp.zeros((MODES, LANES), F32)
    crossed = jnp.zeros((MODES, LANES), F32)
    for c in range(TILES):
        b, part = divmod(c, BS // LANES)
        span = slice(c * LANES, (c + 1) * LANES)
        coupled = coup[span, :].T
        value = image_x[:, span] + coupled[:MODES]
        image_x[:, span] = value
        image_p[:, span] = image_p[:, span] + coupled[MODES:PAIR]
        own = modes[:, span]
        squares += own * own
        crossed += own * value
        kind = kinds[0, first + b]
        line = lines[part][0]
        for other_kind in range(1, NTYPE):
            line = jnp.where(kind == other_kind, lines[part][other_kind], line)
        inverse = 1.0 / (scales[0, first + b] * line)
        ratio = jnp.concatenate([value * inverse, own * inverse], axis=0)
        ratios[:, span] = ratio
        if c < HALO // LANES:
            head[:, span] = ratio
        if c >= TILES - HALO // LANES:
            at = (c - (TILES - HALO // LANES)) * LANES
            tail[:, at : at + LANES] = ratio
    both = jnp.concatenate([squares, crossed, jnp.zeros((LANES - PAIR, LANES), F32)], axis=0)
    total = jnp.sum(both.T, axis=0, keepdims=True)
    sums[...] = jnp.broadcast_to(total, (ALL_DEV, LANES))


def second_kernel(
    gathered, ratios, left, right, other, tables, kinds, scales, rows, rows_o, weights,
    flipped, modes, prev, image_x, image_p, residual, packed,
    blocks, other_t, coup, image_r, gram,
):
    total = jnp.sum(gathered[...], axis=0, keepdims=True)
    column = jnp.broadcast_to(total, (LANES, LANES)).T
    quotient = column[MODES:PAIR, :] / column[:MODES, :]

    def residual_of(source, span):
        return source[:MODES, span] - source[MODES:, span] * quotient

    for c in range(HALO // LANES):
        span = slice(c * LANES, (c + 1) * LANES)
        b, part = divmod(c, BS // LANES)
        lanes = slice(part * LANES, (part + 1) * LANES)
        blocks[b, :MODES, lanes] = residual_of(left, span).astype(BF16)
        blocks[NBR + 2 + b, :MODES, lanes] = residual_of(right, span).astype(BF16)
    for c in range(TILES):
        span = slice(c * LANES, (c + 1) * LANES)
        b, part = divmod(c, BS // LANES)
        lanes = slice(part * LANES, (part + 1) * LANES)
        value = residual_of(ratios, span)
        residual[:, span] = value
        blocks[b + 2, :MODES, lanes] = value.astype(BF16)
        other_t[span, :MODES] = residual_of(other, span).T
    coup[...] = jnp.zeros_like(coup)
    gram[...] = jnp.zeros_like(gram)

    def put(span, value):
        image_r[:, span] = value[:MODES]

    products(blocks, tables, flipped, kinds, scales, rows, rows_o, weights, other_t, coup, put)
    for c in range(TILES):
        span = slice(c * LANES, (c + 1) * LANES)
        image_r[:, span] = image_r[:, span] + coup[span, :].T[:MODES]

    def step(b, carry):
        span = pl.ds(pl.multiple_of(b * BS, BS), BS)
        both = jnp.concatenate(
            [ref[:, span] for ref in (modes, residual, prev, image_x, image_r, image_p)], axis=0
        )
        high = both.astype(BF16)
        low = (both - high.astype(F32)).astype(BF16)
        gram[...] += lax.dot_general(
            jnp.concatenate([high, low], axis=0), high, (((1,), (1,)), ((), ())),
            preferred_element_type=F32,
        )
        return carry

    lax.fori_loop(0, NBR, step, 0)
    n = 3 * MODES
    pad = LANES - n
    zero_r = jnp.zeros((pad, n), F32)
    zero_c = jnp.zeros((LANES, pad), F32)

    def square(top, lane):
        value = gram[top : top + n, lane : lane + n]
        return jnp.concatenate([jnp.concatenate([value, zero_r], axis=0), zero_c], axis=1)

    cross_b = square(2 * n, 0)
    gram_b = square(0, 0) + cross_b + cross_b.T
    cross_a = square(0, n) + square(2 * n, n)
    raw = cross_a + square(3 * n, 0).T
    gram_a = raw + raw.T
    row = lax.broadcasted_iota(jnp.int32, (LANES, LANES), 0)
    col = lax.broadcasted_iota(jnp.int32, (LANES, LANES), 1)
    diagonal = jnp.sum(jnp.where(row == col, gram_a, 0.0), axis=0, keepdims=True)
    merged = jnp.where(row >= col, gram_b, gram_a)
    packed[...] = jnp.where(row == n, jnp.broadcast_to(diagonal, (LANES, LANES)), merged)


def final_kernel(packed, modes, residual, prev, basis, projected, inverse):
    n = 3 * MODES

    @pl.when(pl.program_id(0) == 0)
    def _():
        row = lax.broadcasted_iota(jnp.int32, (LANES, LANES), 0)
        col = lax.broadcasted_iota(jnp.int32, (LANES, LANES), 1)
        merged = packed[...]
        flipped = merged.T
        inside = (row < n) & (col < n)
        ndof = jnp.float32(2.0 * 64 * ROWS)
        gram_b = jnp.where(row >= col, merged, flipped) / ndof
        gram_b = jnp.where(inside, gram_b, jnp.where(row == col, 1.0, 0.0))
        diagonal = jnp.broadcast_to(merged[n : n + 1, :], (LANES, LANES))
        gram_a = jnp.where(row < col, merged, flipped)
        gram_a = jnp.where(row == col, diagonal, gram_a) / (2.0 * ndof)
        gram_a = jnp.where(inside, gram_a, 0.0)
        left = gram_b
        right = jnp.where(row == col, 1.0, 0.0).astype(F32)
        for j in range(n):
            pivot = jnp.broadcast_to(left[:, j : j + 1], (LANES, LANES))
            line_l = left[j : j + 1, :]
            line_r = right[j : j + 1, :]
            root = lax.rsqrt(pivot[j : j + 1, :])
            line_l = line_l * root
            line_r = line_r * root
            factor = jnp.where(row > j, pivot * root, 0.0)
            keep = row == j
            left = jnp.where(keep, line_l, left - factor * line_l)
            right = jnp.where(keep, line_r, right - factor * line_r)
        right = jnp.where(inside, right, 0.0)
        half = lax.dot_general(
            right, gram_a, (((1,), (0,)), ((), ())),
            precision=lax.Precision.HIGHEST, preferred_element_type=F32,
        )
        whole = lax.dot_general(
            half, right, (((1,), (1,)), ((), ())),
            precision=lax.Precision.HIGHEST, preferred_element_type=F32,
        )
        projected[...] = whole[:n, :n]
        inverse[...] = right

    factors = inverse[...][:n, :n]
    high = factors.astype(BF16)
    low = (factors - high.astype(F32)).astype(BF16)
    search = jnp.concatenate([modes[...], residual[...], prev[...]], axis=0)
    search_h = search.astype(BF16)
    search_l = (search - search_h.astype(F32)).astype(BF16)
    top = jnp.concatenate([high, high], axis=1)
    stacked = jnp.concatenate([search_h, search_l], axis=0)
    dims = (((1,), (0,)), ((), ()))
    basis[...] = lax.dot_general(top, stacked, dims, preferred_element_type=F32) + lax.dot_general(
        low, search_h, dims, preferred_element_type=F32
    )


def shards(modes, previous, kinds, scales, tables, wet_rows, wet_counts, coupling):
    modes = modes[0]
    prev = previous[0]
    kinds = kinds[0]
    scales = scales[0]
    tables = tables[0].reshape(3 * NTYPE, BS, BS)
    rows = wet_rows[0]
    used = jnp.arange(IFACE, dtype=jnp.int32) < wet_counts[0]
    weights = jnp.where(used, coupling, jnp.float32(0.0))
    rows_o = swap_field(rows)
    whole, head, tail = rounded_parts(modes, prev)
    rest = (tables, kinds, scales, rows, rows_o, weights)
    rest_specs = [VMEM] + [SMEM] * 5
    plane = shape(MODES, ROWS)
    end = shape(PAIR, HALO)
    image_x, image_p, ratios, head, tail, sums, flipped = pl.pallas_call(
        first_kernel,
        out_shape=(plane, plane, shape(PAIR, ROWS), end, end, shape(ALL_DEV, LANES),
                   shape(2 * NTYPE, BS, BS, kind=BF16)),
        in_specs=[VMEM] * 5 + rest_specs,
        out_specs=[VMEM] * 7,
        scratch_shapes=[
            pltpu.VMEM((NBR + 4, PAIR, BS), BF16),
            pltpu.VMEM((ROWS, LANES), F32),
            pltpu.VMEM((ROWS, LANES), F32),
        ],
        compiler_params=params(28),
        name="first",
    )(modes, prev, from_left(tail), from_right(head), swap_field(whole), *rest)
    gathered = exchange(sums)
    residual, packed = pl.pallas_call(
        second_kernel,
        out_shape=(plane, shape(LANES, LANES)),
        in_specs=[VMEM] * 5 + rest_specs + [VMEM] * 5,
        out_specs=[VMEM] * 2,
        scratch_shapes=[
            pltpu.VMEM((NBR + 4, SINGLE, BS), BF16),
            pltpu.VMEM((ROWS, LANES), F32),
            pltpu.VMEM((ROWS, LANES), F32),
            pltpu.VMEM((MODES, ROWS), F32),
            pltpu.VMEM((12 * MODES, 6 * MODES), F32),
        ],
        compiler_params=params(28),
        name="second",
    )(
        gathered, ratios, from_left(tail), from_right(head), swap_field(ratios), *rest,
        flipped, modes, prev, image_x, image_p,
    )
    part = jnp.sum(exchange(packed), axis=0, keepdims=True)
    packed = exchange(jnp.broadcast_to(part, (ALL_DEV, LANES)))
    width = 1024
    piece = pl.BlockSpec((MODES, width), lambda i: (0, i))
    n = 3 * MODES
    basis, projected = pl.pallas_call(
        final_kernel,
        out_shape=(shape(n, ROWS), shape(n, n)),
        grid=(ROWS // width,),
        in_specs=[pl.BlockSpec((LANES, LANES), lambda i: (0, 0)), piece, piece, piece],
        out_specs=[
            pl.BlockSpec((n, width), lambda i: (0, i)),
            pl.BlockSpec((n, n), lambda i: (0, 0)),
        ],
        scratch_shapes=[pltpu.VMEM((LANES, LANES), F32)],
        compiler_params=params(24),
        name="final",
    )(packed, modes, residual, prev)
    return (basis[None], projected)


def solution(mesh):
    finer = Mesh(
        mesh.devices.reshape(mesh.shape["field"], 4, 4, 4), ("field", "dom_0", "dom_1", "dom_2")
    )
    placed = (
        P("field", None, DOM),
        P("field", None, DOM),
        P("field", None, None),
        P("field", None, None),
        P("field", None, None, None, None),
        P("field", DOM),
        P(DOM),
        P(DOM),
    )
    return jax.shard_map(
        shards, mesh=finer, in_specs=placed, out_specs=(P("field", None, DOM), P()), check_vma=False
    )
```

```python
import functools

import jax
import jax.numpy as jnp
from jax import lax
from jax.experimental import pallas as pl
from jax.experimental.pallas import tpu as pltpu
from jax.sharding import Mesh
from jax.sharding import PartitionSpec as P

BS = 512
NTYPE = 4
NBR = 16
ROWS = NBR * BS
HALO = 2 * BS
MODES = 40
IFACE = 3072
LANES = 128
TILES = ROWS // LANES
DOM = ("dom_0", "dom_1", "dom_2")
FIELD_DOM = ("field", "dom_0", "dom_1", "dom_2")
ALL_DEV = 128
F32 = jnp.float32
BF16 = jnp.bfloat16

VMEM = pl.BlockSpec(memory_space=pltpu.VMEM)
SMEM = pl.BlockSpec(memory_space=pltpu.SMEM)
HBM = pl.BlockSpec(memory_space=pltpu.HBM)
PAIR = 2 * MODES
SINGLE = 48
UNROLL = 2
SLOTS = IFACE // NBR
WIDTH = 1024

OPS = ((0, 0, 0, 0), (1, -1, -1, 0), (2, -2, -2, 0), (1, 1, 0, 1), (2, 2, 0, 1))


def params(mib):
    return pltpu.CompilerParams(vmem_limit_bytes=mib << 20)


def shape(*dims, kind=F32):
    return jax.ShapeDtypeStruct(dims, kind)


def domain_index():
    return (lax.axis_index(DOM[0]) * 4 + lax.axis_index(DOM[1])) * 4 + lax.axis_index(DOM[2])


def in_hbm(value):
    return pltpu.with_memory_space_constraint(value, pltpu.HBM)


def swap_field(value):
    return lax.ppermute(value, "field", [(0, 1), (1, 0)])


def from_left(value):
    return lax.ppermute(value, DOM, [(i, i + 1) for i in range(63)])


def from_right(value):
    return lax.ppermute(value, DOM, [(i + 1, i) for i in range(63)])


def exchange(rows):
    return lax.all_to_all(rows, FIELD_DOM, 0, 0, tiled=True)


def round_kernel(modes, prev, whole, head, tail):
    rounded = jnp.concatenate([modes[...], prev[...]], axis=0).astype(BF16)
    whole[...] = rounded
    head[...] = rounded[:, :HALO]
    tail[...] = rounded[:, ROWS - HALO :]


def rounded_parts(modes, prev):
    end = shape(PAIR, HALO, kind=BF16)
    return pl.pallas_call(
        round_kernel,
        out_shape=(shape(PAIR, ROWS, kind=BF16), end, end),
        in_specs=[VMEM] * 2,
        out_specs=[VMEM] * 3,
        compiler_params=params(24),
        name="rounded",
    )(modes, prev)


def block_sum(b, at, blocks, tables, flipped, kinds, scales):
    first = domain_index() * NBR
    total = None
    for offset, shift, owner, flip in OPS:
        block = jnp.maximum(first + b + owner, 0)
        kind = kinds[offset, block]
        if flip:
            table = flipped[(offset - 1) * NTYPE + kind]
        else:
            table = tables[offset * NTYPE + kind]
        product = jnp.dot(blocks[at + shift], table, preferred_element_type=F32)
        product = scales[offset, block] * product
        total = product if total is None else total + product
    return total


def couple(base, count, rows, rows_o, weights, other_t, coup):
    for v in range(count):
        slot = base + v
        coup[pl.ds(rows[slot], 1), :] = other_t[pl.ds(rows_o[slot], 1), :] * weights[slot]


def inner_kernel(
    modes, prev, other, tables, kinds, scales, rows, rows_o, weights,
    partial_x, partial_p, coup, flipped, blocks, other_t,
):
    for index in range(2 * NTYPE):
        flipped[index] = tables[NTYPE + index].T
    for b in range(NBR):
        span = slice(b * BS, (b + 1) * BS)
        blocks[b] = jnp.concatenate([modes[:, span], prev[:, span]], axis=0).astype(BF16)
    for c in range(TILES):
        span = slice(c * LANES, (c + 1) * LANES)
        other_t[span, :PAIR] = other[:, span].astype(F32).T
    coup[...] = jnp.zeros_like(coup)
    steps = (NBR - 4) // UNROLL
    slots = IFACE // steps

    def step(index, carry):
        for u in range(UNROLL):
            b = 2 + index * UNROLL + u
            total = block_sum(b, b, blocks, tables, flipped, kinds, scales)
            span = pl.ds(pl.multiple_of(b * BS, BS), BS)
            partial_x[:, span] = total[:MODES]
            partial_p[:, span] = total[MODES:]
        couple(index * slots, slots, rows, rows_o, weights, other_t, coup)
        return carry

    lax.fori_loop(0, steps, step, 0)


def outer_kernel(
    modes, prev, left, right, partial_x, partial_p, coup, tables, flipped, kinds, scales,
    image_x, image_p, ratios, head, tail, sums, ends,
):
    first = domain_index() * NBR
    for b in range(2):
        span = slice(b * BS, (b + 1) * BS)
        ends[b] = left[:, span]
        ends[10 + b] = right[:, span]
    for at, b in ((2, 0), (3, 1), (4, 2), (5, 3), (6, 12), (7, 13), (8, 14), (9, 15)):
        span = slice(b * BS, (b + 1) * BS)
        ends[at] = jnp.concatenate([modes[:, span], prev[:, span]], axis=0).astype(BF16)

    def step(index, carry):
        for u in range(2):
            b = index * (NBR - 2) + u
            total = block_sum(b, 2 + index * 6 + u, ends, tables, flipped, kinds, scales)
            span = pl.ds(pl.multiple_of(b * BS, BS), BS)
            partial_x[:, span] = total[:MODES]
            partial_p[:, span] = total[MODES:]
        return carry

    lax.fori_loop(0, 2, step, 0)
    on_diagonal = lax.broadcasted_iota(jnp.int32, (LANES, LANES), 0) == lax.broadcasted_iota(
        jnp.int32, (LANES, LANES), 1
    )
    lines = []
    for part in range(BS // LANES):
        span = slice(part * LANES, (part + 1) * LANES)
        lines.append(
            [
                jnp.sum(
                    jnp.where(on_diagonal, tables[kind, span, span].astype(F32), 0.0),
                    axis=0, keepdims=True,
                )
                for kind in range(NTYPE)
            ]
        )
    squares = jnp.zeros((MODES, LANES), F32)
    crossed = jnp.zeros((MODES, LANES), F32)
    for c in range(TILES):
        b, part = divmod(c, BS // LANES)
        span = slice(c * LANES, (c + 1) * LANES)
        coupled = coup[span, :].T
        value = partial_x[:, span] + coupled[:MODES]
        image_x[:, span] = value
        image_p[:, span] = partial_p[:, span] + coupled[MODES:PAIR]
        own = modes[:, span]
        squares += own * own
        crossed += own * value
        kind = kinds[0, first + b]
        line = lines[part][0]
        for other_kind in range(1, NTYPE):
            line = jnp.where(kind == other_kind, lines[part][other_kind], line)
        inverse = 1.0 / (scales[0, first + b] * line)
        ratio = jnp.concatenate([value * inverse, own * inverse], axis=0)
        ratios[:, span] = ratio
        if c < HALO // LANES:
            head[:, span] = ratio
        if c >= TILES - HALO // LANES:
            at = (c - (TILES - HALO // LANES)) * LANES
            tail[:, at : at + LANES] = ratio
    both = jnp.concatenate([squares, crossed, jnp.zeros((LANES - PAIR, LANES), F32)], axis=0)
    total = jnp.sum(both.T, axis=0, keepdims=True)
    sums[...] = jnp.broadcast_to(total, (ALL_DEV, LANES))


def second_kernel(
    gathered, ratios, left, right, other, tables, kinds, scales, rows, rows_o, weights,
    flipped, modes, prev, image_x, image_p, residual_out, packed,
    blocks, other_t, coup, image_r, gram, residual, sem,
):
    total = jnp.sum(gathered[...], axis=0, keepdims=True)
    column = jnp.broadcast_to(total, (LANES, LANES)).T
    quotient = column[MODES:PAIR, :] / column[:MODES, :]

    def residual_of(source, span):
        return source[:MODES, span] - source[MODES:, span] * quotient

    for c in range(HALO // LANES):
        span = slice(c * LANES, (c + 1) * LANES)
        b, part = divmod(c, BS // LANES)
        lanes = slice(part * LANES, (part + 1) * LANES)
        blocks[b, :MODES, lanes] = residual_of(left, span).astype(BF16)
        blocks[NBR + 2 + b, :MODES, lanes] = residual_of(right, span).astype(BF16)
    for c in range(TILES):
        span = slice(c * LANES, (c + 1) * LANES)
        b, part = divmod(c, BS // LANES)
        lanes = slice(part * LANES, (part + 1) * LANES)
        value = residual_of(ratios, span)
        residual[:, span] = value
        blocks[b + 2, :MODES, lanes] = value.astype(BF16)
        other_t[span, :MODES] = residual_of(other, span).T
    copy = pltpu.make_async_copy(residual, residual_out, sem)
    copy.start()
    coup[...] = jnp.zeros_like(coup)
    gram[...] = jnp.zeros_like(gram)

    def blocked(index, carry):
        for u in range(UNROLL):
            b = index * UNROLL + u
            total = block_sum(b, b + 2, blocks, tables, flipped, kinds, scales)
            image_r[:, pl.ds(pl.multiple_of(b * BS, BS), BS)] = total[:MODES]
        couple(index * UNROLL * SLOTS, UNROLL * SLOTS, rows, rows_o, weights, other_t, coup)
        return carry

    lax.fori_loop(0, NBR // UNROLL, blocked, 0)
    for c in range(TILES):
        span = slice(c * LANES, (c + 1) * LANES)
        image_r[:, span] = image_r[:, span] + coup[span, :].T[:MODES]

    def step(b, carry):
        span = pl.ds(pl.multiple_of(b * BS, BS), BS)
        both = jnp.concatenate(
            [ref[:, span] for ref in (modes, residual, prev, image_x, image_r, image_p)], axis=0
        )
        high = both.astype(BF16)
        low = (both - high.astype(F32)).astype(BF16)
        gram[...] += lax.dot_general(
            jnp.concatenate([high, low], axis=0), high, (((1,), (1,)), ((), ())),
            preferred_element_type=F32,
        )
        return carry

    lax.fori_loop(0, NBR, step, 0)
    n = 3 * MODES
    pad = LANES - n
    zero_r = jnp.zeros((pad, n), F32)
    zero_c = jnp.zeros((LANES, pad), F32)

    def square(top, lane):
        value = gram[top : top + n, lane : lane + n]
        return jnp.concatenate([jnp.concatenate([value, zero_r], axis=0), zero_c], axis=1)

    cross_b = square(2 * n, 0)
    gram_b = square(0, 0) + cross_b + cross_b.T
    cross_a = square(0, n) + square(2 * n, n)
    raw = cross_a + square(3 * n, 0).T
    gram_a = raw + raw.T
    row = lax.broadcasted_iota(jnp.int32, (LANES, LANES), 0)
    col = lax.broadcasted_iota(jnp.int32, (LANES, LANES), 1)
    diagonal = jnp.sum(jnp.where(row == col, gram_a, 0.0), axis=0, keepdims=True)
    merged = jnp.where(row >= col, gram_b, gram_a)
    packed[...] = jnp.where(row == n, jnp.broadcast_to(diagonal, (LANES, LANES)), merged)
    copy.wait()


def lower_inverse(gram, count):
    group = 4
    tiles = count // 8
    sub = lax.broadcasted_iota(jnp.int32, (8, LANES), 0)
    lane = lax.broadcasted_iota(jnp.int32, (8, LANES), 1)
    left = [gram[8 * t : 8 * t + 8, :] for t in range(tiles)]
    right = [jnp.where(lane == sub + 8 * t, 1.0, 0.0).astype(F32) for t in range(tiles)]

    def spread(first):
        return [
            {
                t: jnp.broadcast_to(left[t][:, first + m : first + m + 1], (8, LANES))
                for t in range(first // 8, tiles)
            }
            for m in range(group)
        ]

    ahead = spread(0)
    for start in range(0, count, group):
        now = ahead
        ahead = spread(start + group) if start + group < count else []
        for k in range(group):
            pivot = start + k
            tile, r = divmod(pivot, 8)
            root = lax.rsqrt(now[k][tile][r : r + 1, :])
            factor = {t: now[k][t] * root for t in range(tile, tiles)}
            factor[tile] = jnp.where(sub > r, factor[tile], 0.0)
            for first, columns in ((start, now), (start + group, ahead)):
                for m, column in enumerate(columns):
                    at = first + m
                    if at <= pivot:
                        continue
                    own = factor[at // 8][at % 8 : at % 8 + 1, :]
                    for t in column:
                        column[t] = column[t] - factor[t] * own
            line_l = left[tile][r : r + 1, :] * root
            line_r = right[tile][r : r + 1, :] * root
            for t in range(tile, tiles):
                left[t] = left[t] - factor[t] * line_l
                right[t] = right[t] - factor[t] * line_r
            right[tile] = jnp.where(sub == r, line_r, right[tile])
    return right


def final_kernel(packed, modes, residual_in, prev, basis, projected, result, residual, sems):
    n = 3 * MODES
    load = pltpu.make_async_copy(residual_in, residual, sems.at[ROWS // WIDTH])
    load.start()
    row = lax.broadcasted_iota(jnp.int32, (LANES, LANES), 0)
    col = lax.broadcasted_iota(jnp.int32, (LANES, LANES), 1)
    merged = packed[...]
    flipped = merged.T
    inside = (row < n) & (col < n)
    ndof = jnp.float32(2.0 * 64 * ROWS)
    gram_b = jnp.where(inside, jnp.where(row >= col, merged, flipped) / ndof, 0.0)
    diagonal = jnp.broadcast_to(merged[n : n + 1, :], (LANES, LANES))
    gram_a = jnp.where(row < col, merged, flipped)
    gram_a = jnp.where(row == col, diagonal, gram_a) / (2.0 * ndof)
    gram_a = jnp.where(inside, gram_a, 0.0)
    factors = jnp.concatenate(lower_inverse(gram_b, n), axis=0)
    half = lax.dot_general(
        factors, gram_a, (((1,), (0,)), ((), ())),
        precision=lax.Precision.HIGHEST, preferred_element_type=F32,
    )
    whole = lax.dot_general(
        half, factors, (((1,), (1,)), ((), ())),
        precision=lax.Precision.HIGHEST, preferred_element_type=F32,
    )
    projected[...] = whole
    factors = factors[:, :n]
    high = factors.astype(BF16)
    low = (factors - high.astype(F32)).astype(BF16)
    top = jnp.concatenate([high, high], axis=1)
    dims = (((1,), (0,)), ((), ()))
    load.wait()
    stores = []
    for index in range(ROWS // WIDTH):
        span = pl.ds(index * WIDTH, WIDTH)
        part = jnp.concatenate([modes[:, span], residual[:, span], prev[:, span]], axis=0)
        part_h = part.astype(BF16)
        part_l = (part - part_h.astype(F32)).astype(BF16)
        stacked = jnp.concatenate([part_h, part_l], axis=0)
        result[:, span] = lax.dot_general(
            top, stacked, dims, preferred_element_type=F32
        ) + lax.dot_general(low, part_h, dims, preferred_element_type=F32)
        store = pltpu.make_async_copy(
            result.at[:, span], basis.at[:, span], sems.at[index]
        )
        store.start()
        stores.append(store)
    for store in stores:
        store.wait()


def shards(modes, previous, kinds, scales, tables, wet_rows, wet_counts, coupling):
    modes = modes[0]
    prev = previous[0]
    kinds = kinds[0]
    scales = scales[0]
    tables = tables[0].reshape(3 * NTYPE, BS, BS)
    rows = wet_rows[0]
    used = jnp.arange(IFACE, dtype=jnp.int32) < wet_counts[0]
    weights = jnp.where(used, coupling, jnp.float32(0.0))
    rows_o = swap_field(rows)
    whole, head, tail = rounded_parts(modes, prev)
    left, right, other = from_left(tail), from_right(head), swap_field(whole)
    coupling_args = (rows, rows_o, weights)
    plane = shape(MODES, ROWS)
    rows_by_lanes = shape(ROWS, LANES)
    end = shape(PAIR, HALO)
    partial_x, partial_p, coup, flipped = pl.pallas_call(
        inner_kernel,
        out_shape=(plane, plane, rows_by_lanes, shape(2 * NTYPE, BS, BS, kind=BF16)),
        in_specs=[VMEM] * 4 + [SMEM] * 5,
        out_specs=[VMEM] * 4,
        scratch_shapes=[
            pltpu.VMEM((NBR, PAIR, BS), BF16),
            pltpu.VMEM((ROWS, LANES), F32),
        ],
        compiler_params=params(10),
        name="inner",
    )(modes, prev, other, tables, kinds, scales, *coupling_args)
    image_x, image_p, ratios, head, tail, sums = pl.pallas_call(
        outer_kernel,
        out_shape=(plane, plane, shape(PAIR, ROWS), end, end, shape(ALL_DEV, LANES)),
        in_specs=[VMEM] * 9 + [SMEM] * 2,
        out_specs=[VMEM] * 6,
        scratch_shapes=[pltpu.VMEM((12, PAIR, BS), BF16)],
        compiler_params=params(6),
        name="outer",
    )(modes, prev, left, right, partial_x, partial_p, coup, tables, flipped, kinds, scales)
    gathered = exchange(sums)
    residual, packed = pl.pallas_call(
        second_kernel,
        out_shape=(pltpu.HBM((MODES, ROWS), F32), shape(LANES, LANES)),
        in_specs=[VMEM] * 6 + [SMEM] * 5 + [VMEM] * 5,
        out_specs=[HBM, VMEM],
        scratch_shapes=[
            pltpu.VMEM((NBR + 4, SINGLE, BS), BF16),
            pltpu.VMEM((ROWS, LANES), F32),
            pltpu.VMEM((ROWS, LANES), F32),
            pltpu.VMEM((MODES, ROWS), F32),
            pltpu.VMEM((12 * MODES, 6 * MODES), F32),
            pltpu.VMEM((MODES, ROWS), F32),
            pltpu.SemaphoreType.DMA(()),
        ],
        compiler_params=params(18),
        name="second",
    )(
        gathered, ratios, from_left(tail), from_right(head), swap_field(ratios),
        tables, kinds, scales, *coupling_args,
        flipped, modes, prev, image_x, image_p,
    )
    part = jnp.sum(exchange(packed), axis=0, keepdims=True)
    packed = exchange(jnp.broadcast_to(part, (ALL_DEV, LANES)))
    n = 3 * MODES
    basis, projected = pl.pallas_call(
        final_kernel,
        out_shape=(pltpu.HBM((n, ROWS), F32), shape(n, n)),
        in_specs=[VMEM, VMEM, HBM, VMEM],
        out_specs=[HBM, VMEM],
        scratch_shapes=[
            pltpu.VMEM((n, ROWS), F32),
            pltpu.VMEM((MODES, ROWS), F32),
            pltpu.SemaphoreType.DMA((ROWS // WIDTH + 1,)),
        ],
        compiler_params=params(14),
        name="final",
    )(packed, modes, in_hbm(residual), prev)
    return (basis[None], projected)


def solution(mesh):
    finer = Mesh(
        mesh.devices.reshape(mesh.shape["field"], 4, 4, 4), ("field", "dom_0", "dom_1", "dom_2")
    )
    placed = (
        P("field", None, DOM),
        P("field", None, DOM),
        P("field", None, None),
        P("field", None, None),
        P("field", None, None, None, None),
        P("field", DOM),
        P(DOM),
        P(DOM),
    )
    return jax.shard_map(
        shards, mesh=finer, in_specs=placed, out_specs=(P("field", None, DOM), P()), check_vma=False
    )
```

```python
import jax
import jax.numpy as jnp
from jax import lax
from jax.experimental import pallas as pl
from jax.experimental.pallas import tpu as pltpu
from jax.sharding import Mesh
from jax.sharding import PartitionSpec as P


BS = 512
NTYPE = 4
NBR = 16
NBLK = 1024
ROWS = NBR * BS
HALO = 2 * BS
MODES = 40
IFACE = 3072
LANES = 128
TILES = ROWS // LANES
DOM = ("dom_0", "dom_1", "dom_2")
FIELD_DOM = ("field", "dom_0", "dom_1", "dom_2")
ALL_DEV = 128
F32 = jnp.float32
BF16 = jnp.bfloat16

VMEM = pl.BlockSpec(memory_space=pltpu.VMEM)
SMEM = pl.BlockSpec(memory_space=pltpu.SMEM)
HBM = pl.BlockSpec(memory_space=pltpu.HBM)
PAIR = 2 * MODES
SINGLE = 48
UNROLL = 2
SLOTS = IFACE // NBR
WIDTH = 1024

OPS = ((0, 0, 0, 0), (1, -1, -1, 0), (2, -2, -2, 0), (1, 1, 0, 1), (2, 2, 0, 1))


def params(mib):
    return pltpu.CompilerParams(vmem_limit_bytes=mib << 20)


def shape(*dims, kind=F32):
    return jax.ShapeDtypeStruct(dims, kind)


def domain_index():
    return (lax.axis_index(DOM[0]) * 4 + lax.axis_index(DOM[1])) * 4 + lax.axis_index(DOM[2])


def in_hbm(value):
    return pltpu.with_memory_space_constraint(value, pltpu.HBM)


def swap_field(value):
    return lax.ppermute(value, "field", [(0, 1), (1, 0)])


def from_left(value):
    return lax.ppermute(value, DOM, [(i, i + 1) for i in range(63)])


def from_right(value):
    return lax.ppermute(value, DOM, [(i + 1, i) for i in range(63)])


def exchange(rows):
    return lax.all_to_all(rows, FIELD_DOM, 0, 0, tiled=True)


def round_kernel(
    modes, prev, coupling, rows, counts,
    modes_v, prev_v, whole, head, tail, weights, rows_v, sems,
):
    pairs = ((modes, modes_v), (prev, prev_v), (coupling, weights), (rows, rows_v))
    loads = [
        pltpu.make_async_copy(source, target, sems.at[index])
        for index, (source, target) in enumerate(pairs)
    ]
    for load in loads:
        load.start()
    slot = lax.broadcasted_iota(jnp.int32, weights.shape, 0) * LANES + lax.broadcasted_iota(
        jnp.int32, weights.shape, 1
    )
    for load in loads:
        load.wait()
    weights[...] = jnp.where(slot < counts[0], weights[...], 0.0)
    rounded = jnp.concatenate([modes_v[...], prev_v[...]], axis=0).astype(BF16)
    whole[...] = rounded
    head[...] = rounded[:, :HALO]
    tail[...] = rounded[:, ROWS - HALO :]


def rounded_parts(modes, prev, coupling, rows, counts):
    plane = shape(MODES, ROWS)
    end = shape(PAIR, HALO, kind=BF16)
    slots = shape(IFACE // LANES, LANES)
    return pl.pallas_call(
        round_kernel,
        out_shape=(plane, plane, shape(PAIR, ROWS, kind=BF16), end, end, slots,
                   shape(IFACE // LANES, LANES, kind=jnp.int32)),
        in_specs=[HBM] * 4 + [SMEM],
        out_specs=[VMEM] * 7,
        scratch_shapes=[pltpu.SemaphoreType.DMA((4,))],
        compiler_params=params(12),
        name="rounded",
    )(
        *map(in_hbm, (modes, prev, coupling.reshape(slots.shape), rows.reshape(slots.shape))),
        counts,
    )


def block_sum(b, at, blocks, tables, flipped, kinds, scales, beside=None):
    first = domain_index() * NBR
    total = None
    for index, (offset, shift, owner, flip) in enumerate(OPS):
        block = offset * NBLK + jnp.maximum(first + b + owner, 0)
        kind = kinds[block]
        if flip:
            table = flipped[(offset - 1) * NTYPE + kind]
        else:
            table = tables[offset * NTYPE + kind]
        product = jnp.dot(blocks[at + shift], table, preferred_element_type=F32)
        if beside is not None:
            beside(index, product[0, 0])
        product = scales[block] * product
        total = product if total is None else total + product
    return total


def coupler(base, total, dots, rows, rows_o, weights, other_t, coup):
    share = total // dots
    taken = []

    def beside(_, value):
        if len(taken) == dots:
            return
        late = jnp.where(value == value, 0, 1)
        start = jnp.minimum(base + len(taken) * share + late, IFACE - share)
        taken.append(start)
        for v in range(share):
            slot = start + v
            coup[pl.ds(rows[slot], 1), :] = other_t[pl.ds(rows_o[slot], 1), :] * weights[slot]

    return beside


def inner_kernel(
    modes, prev, other, tables_in, kinds, scales, rows, rows_o, weights,
    partial_x, partial_p, coup, tables, flipped, blocks, other_t, sem,
):
    load = pltpu.make_async_copy(tables_in, tables, sem)
    load.start()
    for b in range(NBR):
        span = slice(b * BS, (b + 1) * BS)
        blocks[b] = jnp.concatenate([modes[:, span], prev[:, span]], axis=0).astype(BF16)
    for c in range(TILES):
        span = slice(c * LANES, (c + 1) * LANES)
        other_t[span, :PAIR] = other[:, span].astype(F32).T
    coup[...] = jnp.zeros_like(coup)
    load.wait()
    for index in range(2 * NTYPE):
        flipped[index] = tables[NTYPE + index].T
    steps = (NBR - 4) // UNROLL
    slots = IFACE // steps

    def step(index, carry):
        beside = coupler(index * slots, slots, 8, rows, rows_o, weights, other_t, coup)
        for u in range(UNROLL):
            b = 2 + index * UNROLL + u
            total = block_sum(b, b, blocks, tables, flipped, kinds, scales, beside)
            span = pl.ds(pl.multiple_of(b * BS, BS), BS)
            partial_x[:, span] = total[:MODES]
            partial_p[:, span] = total[MODES:]
        return carry

    lax.fori_loop(0, steps, step, 0)


def outer_kernel(
    modes, prev, left, right, partial_x, partial_p, coup, tables, flipped, kinds, scales,
    image_x, image_p, ratios, head, tail, sums, ends,
):
    first = domain_index() * NBR
    for b in range(2):
        span = slice(b * BS, (b + 1) * BS)
        ends[b] = left[:, span]
        ends[10 + b] = right[:, span]
    for at, b in ((2, 0), (3, 1), (4, 2), (5, 3), (6, 12), (7, 13), (8, 14), (9, 15)):
        span = slice(b * BS, (b + 1) * BS)
        ends[at] = jnp.concatenate([modes[:, span], prev[:, span]], axis=0).astype(BF16)

    def step(index, carry):
        for u in range(2):
            b = index * (NBR - 2) + u
            total = block_sum(b, 2 + index * 6 + u, ends, tables, flipped, kinds, scales)
            span = pl.ds(pl.multiple_of(b * BS, BS), BS)
            partial_x[:, span] = total[:MODES]
            partial_p[:, span] = total[MODES:]
        return carry

    lax.fori_loop(0, 2, step, 0)
    on_diagonal = lax.broadcasted_iota(jnp.int32, (LANES, LANES), 0) == lax.broadcasted_iota(
        jnp.int32, (LANES, LANES), 1
    )
    lines = []
    for part in range(BS // LANES):
        span = slice(part * LANES, (part + 1) * LANES)
        lines.append(
            [
                jnp.sum(
                    jnp.where(on_diagonal, tables[kind, span, span].astype(F32), 0.0),
                    axis=0, keepdims=True,
                )
                for kind in range(NTYPE)
            ]
        )
    squares = jnp.zeros((MODES, LANES), F32)
    crossed = jnp.zeros((MODES, LANES), F32)
    for c in range(TILES):
        b, part = divmod(c, BS // LANES)
        span = slice(c * LANES, (c + 1) * LANES)
        coupled = coup[span, :].T
        value = partial_x[:, span] + coupled[:MODES]
        image_x[:, span] = value
        image_p[:, span] = partial_p[:, span] + coupled[MODES:PAIR]
        own = modes[:, span]
        squares += own * own
        crossed += own * value
        kind = kinds[first + b]
        line = lines[part][0]
        for other_kind in range(1, NTYPE):
            line = jnp.where(kind == other_kind, lines[part][other_kind], line)
        inverse = 1.0 / (scales[first + b] * line)
        ratio = jnp.concatenate([value * inverse, own * inverse], axis=0)
        ratios[:, span] = ratio
        if c < HALO // LANES:
            head[:, span] = ratio
        if c >= TILES - HALO // LANES:
            at = (c - (TILES - HALO // LANES)) * LANES
            tail[:, at : at + LANES] = ratio
    both = jnp.concatenate([squares, crossed, jnp.zeros((LANES - PAIR, LANES), F32)], axis=0)
    total = jnp.sum(both.T, axis=0, keepdims=True)
    sums[...] = jnp.broadcast_to(total, (ALL_DEV, LANES))


def second_kernel(
    gathered, ratios, left, right, other, tables, kinds, scales, rows, rows_o, weights,
    flipped, modes, prev, image_x, image_p, residual_out, packed,
    blocks, other_t, coup, image_r, gram, residual, sem,
):
    total = jnp.sum(gathered[...], axis=0, keepdims=True)
    column = jnp.broadcast_to(total, (LANES, LANES)).T
    quotient = column[MODES:PAIR, :] / column[:MODES, :]

    def residual_of(source, span):
        return source[:MODES, span] - source[MODES:, span] * quotient

    for c in range(HALO // LANES):
        span = slice(c * LANES, (c + 1) * LANES)
        b, part = divmod(c, BS // LANES)
        lanes = slice(part * LANES, (part + 1) * LANES)
        blocks[b, :MODES, lanes] = residual_of(left, span).astype(BF16)
        blocks[NBR + 2 + b, :MODES, lanes] = residual_of(right, span).astype(BF16)
    for c in range(TILES):
        span = slice(c * LANES, (c + 1) * LANES)
        b, part = divmod(c, BS // LANES)
        lanes = slice(part * LANES, (part + 1) * LANES)
        value = residual_of(ratios, span)
        residual[:, span] = value
        blocks[b + 2, :MODES, lanes] = value.astype(BF16)
        other_t[span, :MODES] = residual_of(other, span).T
    copy = pltpu.make_async_copy(residual, residual_out, sem)
    copy.start()
    coup[...] = jnp.zeros_like(coup)
    gram[...] = jnp.zeros_like(gram)

    def blocked(index, carry):
        slots = UNROLL * SLOTS
        beside = coupler(index * slots, slots, 8, rows, rows_o, weights, other_t, coup)
        for u in range(UNROLL):
            b = index * UNROLL + u
            total = block_sum(b, b + 2, blocks, tables, flipped, kinds, scales, beside)
            image_r[:, pl.ds(pl.multiple_of(b * BS, BS), BS)] = total[:MODES]
        return carry

    lax.fori_loop(0, NBR // UNROLL, blocked, 0)
    for c in range(TILES):
        span = slice(c * LANES, (c + 1) * LANES)
        image_r[:, span] = image_r[:, span] + coup[span, :].T[:MODES]

    def step(b, carry):
        span = pl.ds(pl.multiple_of(b * 2 * BS, 2 * BS), 2 * BS)
        both = jnp.concatenate(
            [ref[:, span] for ref in (modes, residual, prev, image_x, image_r, image_p)], axis=0
        )
        high = both.astype(BF16)
        low = (both - high.astype(F32)).astype(BF16)
        gram[...] += lax.dot_general(
            jnp.concatenate([high, low], axis=0), high, (((1,), (1,)), ((), ())),
            preferred_element_type=F32,
        )
        return carry

    lax.fori_loop(0, NBR // 2, step, 0)
    n = 3 * MODES
    pad = LANES - n
    zero_r = jnp.zeros((pad, n), F32)
    zero_c = jnp.zeros((LANES, pad), F32)

    def square(top, lane):
        value = gram[top : top + n, lane : lane + n]
        return jnp.concatenate([jnp.concatenate([value, zero_r], axis=0), zero_c], axis=1)

    cross_b = square(2 * n, 0)
    gram_b = square(0, 0) + cross_b + cross_b.T
    cross_a = square(0, n) + square(2 * n, n)
    raw = cross_a + square(3 * n, 0).T
    gram_a = raw + raw.T
    row = lax.broadcasted_iota(jnp.int32, (LANES, LANES), 0)
    col = lax.broadcasted_iota(jnp.int32, (LANES, LANES), 1)
    diagonal = jnp.sum(jnp.where(row == col, gram_a, 0.0), axis=0, keepdims=True)
    merged = jnp.where(row >= col, gram_b, gram_a)
    packed[...] = jnp.where(row == n, jnp.broadcast_to(diagonal, (LANES, LANES)), merged)
    copy.wait()


def lower_inverse(gram, count):
    group = 4
    tiles = count // 8
    sub = lax.broadcasted_iota(jnp.int32, (8, LANES), 0)
    lane = lax.broadcasted_iota(jnp.int32, (8, LANES), 1)
    left = [gram[8 * t : 8 * t + 8, :] for t in range(tiles)]
    right = [jnp.where(lane == sub + 8 * t, 1.0, 0.0).astype(F32) for t in range(tiles)]

    def spread(first):
        return [
            {
                t: jnp.broadcast_to(left[t][:, first + m : first + m + 1], (8, LANES))
                for t in range(first // 8, tiles)
            }
            for m in range(group)
        ]

    ahead = spread(0)
    for start in range(0, count, group):
        now = ahead
        ahead = spread(start + group) if start + group < count else []
        for k in range(group):
            pivot = start + k
            tile, r = divmod(pivot, 8)
            root = lax.rsqrt(now[k][tile][r : r + 1, :])
            factor = {t: now[k][t] * root for t in range(tile, tiles)}
            factor[tile] = jnp.where(sub > r, factor[tile], 0.0)
            for first, columns in ((start, now), (start + group, ahead)):
                for m, column in enumerate(columns):
                    at = first + m
                    if at <= pivot:
                        continue
                    own = factor[at // 8][at % 8 : at % 8 + 1, :]
                    for t in column:
                        column[t] = column[t] - factor[t] * own
            line_l = left[tile][r : r + 1, :] * root
            line_r = right[tile][r : r + 1, :] * root
            for t in range(tile, tiles):
                left[t] = left[t] - factor[t] * line_l
                right[t] = right[t] - factor[t] * line_r
            right[tile] = jnp.where(sub == r, line_r, right[tile])
    return right


def final_kernel(packed, modes, residual_in, prev, basis, projected, result, residual, sems):
    n = 3 * MODES
    load = pltpu.make_async_copy(residual_in, residual, sems.at[ROWS // WIDTH])
    load.start()
    row = lax.broadcasted_iota(jnp.int32, (LANES, LANES), 0)
    col = lax.broadcasted_iota(jnp.int32, (LANES, LANES), 1)
    merged = packed[...]
    flipped = merged.T
    inside = (row < n) & (col < n)
    ndof = jnp.float32(2.0 * 64 * ROWS)
    gram_b = jnp.where(inside, jnp.where(row >= col, merged, flipped) / ndof, 0.0)
    diagonal = jnp.broadcast_to(merged[n : n + 1, :], (LANES, LANES))
    gram_a = jnp.where(row < col, merged, flipped)
    gram_a = jnp.where(row == col, diagonal, gram_a) / (2.0 * ndof)
    gram_a = jnp.where(inside, gram_a, 0.0)
    factors = jnp.concatenate(lower_inverse(gram_b, n), axis=0)
    half = lax.dot_general(
        factors, gram_a, (((1,), (0,)), ((), ())),
        precision=lax.Precision.HIGHEST, preferred_element_type=F32,
    )
    whole = lax.dot_general(
        half, factors, (((1,), (1,)), ((), ())),
        precision=lax.Precision.HIGHEST, preferred_element_type=F32,
    )
    projected[...] = whole
    factors = factors[:, :n]
    high = factors.astype(BF16)
    low = (factors - high.astype(F32)).astype(BF16)
    top = jnp.concatenate([high, high], axis=1)
    dims = (((1,), (0,)), ((), ()))
    load.wait()
    stores = []
    for index in range(ROWS // WIDTH):
        span = pl.ds(index * WIDTH, WIDTH)
        part = jnp.concatenate([modes[:, span], residual[:, span], prev[:, span]], axis=0)
        part_h = part.astype(BF16)
        part_l = (part - part_h.astype(F32)).astype(BF16)
        stacked = jnp.concatenate([part_h, part_l], axis=0)
        result[:, span] = lax.dot_general(
            top, stacked, dims, preferred_element_type=F32
        ) + lax.dot_general(low, part_h, dims, preferred_element_type=F32)
        store = pltpu.make_async_copy(
            result.at[:, span], basis.at[:, span], sems.at[index]
        )
        store.start()
        stores.append(store)
    for store in stores:
        store.wait()


def shards(modes, previous, kinds, scales, tables, wet_rows, wet_counts, coupling):
    modes = modes[0]
    prev = previous[0]
    kinds = kinds[0].reshape(3 * NBLK)
    scales = scales[0].reshape(3 * NBLK)
    tables = tables[0].reshape(3 * NTYPE, BS, BS)
    rows = wet_rows[0]
    modes, prev, whole, head, tail, weights, rows = rounded_parts(
        modes, prev, coupling, rows, wet_counts
    )
    weights = weights.reshape(IFACE)
    rows_o = swap_field(rows).reshape(IFACE)
    rows = rows.reshape(IFACE)
    other = swap_field(whole)
    left = from_left(tail)
    right = from_right(head)
    coupling_args = (rows, rows_o, weights)
    plane = shape(MODES, ROWS)
    rows_by_lanes = shape(ROWS, LANES)
    end = shape(PAIR, HALO)
    partial_x, partial_p, coup, tables, flipped = pl.pallas_call(
        inner_kernel,
        out_shape=(
            plane, plane, rows_by_lanes,
            shape(3 * NTYPE, BS, BS, kind=BF16), shape(2 * NTYPE, BS, BS, kind=BF16),
        ),
        in_specs=[VMEM] * 3 + [HBM] + [SMEM] * 5,
        out_specs=[VMEM] * 5,
        scratch_shapes=[
            pltpu.VMEM((NBR, PAIR, BS), BF16),
            pltpu.VMEM((ROWS, LANES), F32),
            pltpu.SemaphoreType.DMA(()),
        ],
        compiler_params=params(10),
        name="inner",
    )(modes, prev, other, in_hbm(tables), kinds, scales, *coupling_args)
    image_x, image_p, ratios, head, tail, sums = pl.pallas_call(
        outer_kernel,
        out_shape=(plane, plane, shape(PAIR, ROWS), end, end, shape(ALL_DEV, LANES)),
        in_specs=[VMEM] * 9 + [SMEM] * 2,
        out_specs=[VMEM] * 6,
        scratch_shapes=[pltpu.VMEM((12, PAIR, BS), BF16)],
        compiler_params=params(6),
        name="outer",
    )(modes, prev, left, right, partial_x, partial_p, coup, tables, flipped, kinds, scales)
    gathered = exchange(sums)
    residual, packed = pl.pallas_call(
        second_kernel,
        out_shape=(pltpu.HBM((MODES, ROWS), F32), shape(LANES, LANES)),
        in_specs=[VMEM] * 6 + [SMEM] * 5 + [VMEM] * 5,
        out_specs=[HBM, VMEM],
        scratch_shapes=[
            pltpu.VMEM((NBR + 4, SINGLE, BS), BF16),
            pltpu.VMEM((ROWS, LANES), F32),
            pltpu.VMEM((ROWS, LANES), F32),
            pltpu.VMEM((MODES, ROWS), F32),
            pltpu.VMEM((12 * MODES, 6 * MODES), F32),
            pltpu.VMEM((MODES, ROWS), F32),
            pltpu.SemaphoreType.DMA(()),
        ],
        compiler_params=params(18),
        name="second",
    )(
        gathered, ratios, from_left(tail), from_right(head), swap_field(ratios),
        tables, kinds, scales, *coupling_args,
        flipped, modes, prev, image_x, image_p,
    )
    part = jnp.sum(exchange(packed), axis=0, keepdims=True)
    packed = exchange(jnp.broadcast_to(part, (ALL_DEV, LANES)))
    n = 3 * MODES
    basis, projected = pl.pallas_call(
        final_kernel,
        out_shape=(pltpu.HBM((n, ROWS), F32), shape(n, n)),
        in_specs=[VMEM, VMEM, HBM, VMEM],
        out_specs=[HBM, VMEM],
        scratch_shapes=[
            pltpu.VMEM((n, ROWS), F32),
            pltpu.VMEM((MODES, ROWS), F32),
            pltpu.SemaphoreType.DMA((ROWS // WIDTH + 1,)),
        ],
        compiler_params=params(14),
        name="final",
    )(packed, modes, in_hbm(residual), prev)
    return (basis[None], projected)


def solution(mesh):
    finer = Mesh(
        mesh.devices.reshape(mesh.shape["field"], 4, 4, 4), ("field", "dom_0", "dom_1", "dom_2")
    )
    placed = (
        P("field", None, DOM),
        P("field", None, DOM),
        P("field", None, None),
        P("field", None, None),
        P("field", None, None, None, None),
        P("field", DOM),
        P(DOM),
        P(DOM),
    )
    return jax.shard_map(
        shards, mesh=finer, in_specs=placed, out_specs=(P("field", None, DOM), P()), check_vma=False
    )
```

```python
import jax
import jax.numpy as jnp
from jax import lax
from jax.experimental import pallas as pl
from jax.experimental.pallas import tpu as pltpu
from jax.sharding import Mesh
from jax.sharding import PartitionSpec as P


BS = 512
NTYPE = 4
NBR = 16
NBLK = 1024
ROWS = NBR * BS
HALO = 2 * BS
MODES = 40
IFACE = 3072
LANES = 128
TILES = ROWS // LANES
DOM = ("dom_0", "dom_1", "dom_2")
FIELD_DOM = ("field", "dom_0", "dom_1", "dom_2")
ALL_DEV = 128
F32 = jnp.float32
BF16 = jnp.bfloat16

VMEM = pl.BlockSpec(memory_space=pltpu.VMEM)
SMEM = pl.BlockSpec(memory_space=pltpu.SMEM)
HBM = pl.BlockSpec(memory_space=pltpu.HBM)
PAIR = 2 * MODES
SINGLE = 48
INNER = 6
ENDS = ((2, 0), (3, 1), (4, 2), (5, 3), (6, 12), (7, 13), (8, 14), (9, 15))
WIDTH = 1024

OPS = ((0, 0, 0, 0), (1, -1, -1, 0), (2, -2, -2, 0), (1, 1, 0, 1), (2, 2, 0, 1))


def params(mib):
    return pltpu.CompilerParams(vmem_limit_bytes=mib << 20)


def shape(*dims, kind=F32):
    return jax.ShapeDtypeStruct(dims, kind)


def domain_index():
    return (lax.axis_index(DOM[0]) * 4 + lax.axis_index(DOM[1])) * 4 + lax.axis_index(DOM[2])


def in_hbm(value):
    return pltpu.with_memory_space_constraint(value, pltpu.HBM)


def swap_field(value):
    return lax.ppermute(value, "field", [(0, 1), (1, 0)])


def from_left(value):
    return lax.ppermute(value, DOM, [(i, i + 1) for i in range(63)])


def from_right(value):
    return lax.ppermute(value, DOM, [(i + 1, i) for i in range(63)])


def exchange(rows):
    return lax.all_to_all(rows, FIELD_DOM, 0, 0, tiled=True)


def round_kernel(
    modes, prev, coupling, rows, counts,
    modes_v, prev_v, whole, head, tail, weights, rows_v, sems,
):
    pairs = ((modes, modes_v), (prev, prev_v), (coupling, weights), (rows, rows_v))
    loads = [
        pltpu.make_async_copy(source, target, sems.at[index])
        for index, (source, target) in enumerate(pairs)
    ]
    for load in loads:
        load.start()
    slot = lax.broadcasted_iota(jnp.int32, weights.shape, 0) * LANES + lax.broadcasted_iota(
        jnp.int32, weights.shape, 1
    )
    for load in loads:
        load.wait()
    weights[...] = jnp.where(slot < counts[0], weights[...], 0.0)
    rounded = jnp.concatenate([modes_v[...], prev_v[...]], axis=0).astype(BF16)
    whole[...] = rounded
    head[...] = rounded[:, :HALO]
    tail[...] = rounded[:, ROWS - HALO :]


def rounded_parts(modes, prev, coupling, rows, counts):
    plane = shape(MODES, ROWS)
    end = shape(PAIR, HALO, kind=BF16)
    slots = shape(IFACE // LANES, LANES)
    return pl.pallas_call(
        round_kernel,
        out_shape=(plane, plane, shape(PAIR, ROWS, kind=BF16), end, end, slots,
                   shape(IFACE // LANES, LANES, kind=jnp.int32)),
        in_specs=[HBM] * 4 + [SMEM],
        out_specs=[VMEM] * 7,
        scratch_shapes=[pltpu.SemaphoreType.DMA((4,))],
        compiler_params=params(12),
        name="rounded",
    )(
        *map(in_hbm, (modes, prev, coupling.reshape(slots.shape), rows.reshape(slots.shape))),
        counts,
    )


def block_sum(b, at, blocks, tables, flipped, kinds, scales, beside=None):
    first = domain_index() * NBR
    total = None
    for index, (offset, shift, owner, flip) in enumerate(OPS):
        block = offset * NBLK + jnp.maximum(first + b + owner, 0)
        kind = kinds[block]
        if flip:
            table = flipped[(offset - 1) * NTYPE + kind]
        else:
            table = tables[offset * NTYPE + kind]
        product = jnp.dot(blocks[at + shift], table, preferred_element_type=F32)
        if beside is not None:
            beside(index, product[0, 0])
        product = scales[block] * product
        total = product if total is None else total + product
    return total


def coupler(base, total, dots, rows, rows_o, weights, other_t, coup):
    cuts = [total * index // dots for index in range(dots + 1)]
    taken = []

    def beside(_, value):
        if len(taken) == dots:
            return
        late = jnp.where(value == value, 0, 1)
        cut, share = cuts[len(taken)], cuts[len(taken) + 1] - cuts[len(taken)]
        start = jnp.minimum(base + cut + late, IFACE - share)
        taken.append(start)
        for v in range(share):
            slot = start + v
            coup[pl.ds(rows[slot], 1), :] = other_t[pl.ds(rows_o[slot], 1), :] * weights[slot]

    return beside


def inner_kernel(
    modes, prev, other, tables_in, kinds, scales, rows, rows_o, weights,
    partial_x, partial_p, coup, tables, flipped, blocks, other_t, sems,
):
    loads = [
        pltpu.make_async_copy(
            tables_in.at[pl.ds(offset * NTYPE, NTYPE)],
            tables.at[pl.ds(offset * NTYPE, NTYPE)],
            sems.at[offset],
        )
        for offset in range(3)
    ]
    for offset in (1, 2, 0):
        loads[offset].start()
    for b in range(NBR):
        span = slice(b * BS, (b + 1) * BS)
        blocks[b] = jnp.concatenate([modes[:, span], prev[:, span]], axis=0).astype(BF16)
    for c in range(TILES):
        span = slice(c * LANES, (c + 1) * LANES)
        other_t[span, :PAIR] = other[:, span].astype(F32).T
    coup[...] = jnp.zeros_like(coup)
    for offset in (1, 2):
        loads[offset].wait()
        for index in range(NTYPE):
            flipped[(offset - 1) * NTYPE + index] = tables[offset * NTYPE + index].T
    loads[0].wait()
    steps = (NBR - 4) // INNER
    slots = IFACE // steps

    def step(index, carry):
        beside = coupler(index * slots, slots, 5 * INNER - 1, rows, rows_o, weights, other_t, coup)
        for u in range(INNER):
            b = 2 + index * INNER + u
            total = block_sum(b, b, blocks, tables, flipped, kinds, scales, beside)
            span = pl.ds(pl.multiple_of(b * BS, BS), BS)
            partial_x[:, span] = total[:MODES]
            partial_p[:, span] = total[MODES:]
        return carry

    lax.fori_loop(0, steps, step, 0)


def outer_kernel(
    modes, prev, left, right, partial_x, partial_p, coup, tables, flipped, kinds, scales,
    image_x, image_p, inverse_j, sums, ends,
):
    first = domain_index() * NBR
    for b in range(2):
        span = slice(b * BS, (b + 1) * BS)
        ends[b] = left[:, span]
        ends[10 + b] = right[:, span]
    for at, b in ENDS:
        span = slice(b * BS, (b + 1) * BS)
        ends[at] = jnp.concatenate([modes[:, span], prev[:, span]], axis=0).astype(BF16)

    def step(index, carry):
        for u in range(2):
            b = index * (NBR - 2) + u
            total = block_sum(b, 2 + index * 6 + u, ends, tables, flipped, kinds, scales)
            span = pl.ds(pl.multiple_of(b * BS, BS), BS)
            image_x[:, span] = total[:MODES]
            image_p[:, span] = total[MODES:]
        return carry

    lax.fori_loop(0, 2, step, 0)
    on_diagonal = lax.broadcasted_iota(jnp.int32, (LANES, LANES), 0) == lax.broadcasted_iota(
        jnp.int32, (LANES, LANES), 1
    )
    lines = []
    for part in range(BS // LANES):
        span = slice(part * LANES, (part + 1) * LANES)
        lines.append(
            [
                jnp.sum(
                    jnp.where(on_diagonal, tables[kind, span, span].astype(F32), 0.0),
                    axis=0, keepdims=True,
                )
                for kind in range(NTYPE)
            ]
        )
    squares = jnp.zeros((MODES, LANES), F32)
    crossed = jnp.zeros((MODES, LANES), F32)
    for c in range(TILES):
        b, part = divmod(c, BS // LANES)
        span = slice(c * LANES, (c + 1) * LANES)
        coupled = coup[span, :].T
        source_x, source_p = (partial_x, partial_p) if 2 <= b < NBR - 2 else (image_x, image_p)
        value = source_x[:, span] + coupled[:MODES]
        image_x[:, span] = value
        image_p[:, span] = source_p[:, span] + coupled[MODES:PAIR]
        own = modes[:, span]
        squares += own * own
        crossed += own * value
        kind = kinds[first + b]
        line = lines[part][0]
        for other_kind in range(1, NTYPE):
            line = jnp.where(kind == other_kind, lines[part][other_kind], line)
        inverse_j[:, span] = 1.0 / (scales[first + b] * line)
    both = jnp.concatenate([squares, crossed, jnp.zeros((LANES - PAIR, LANES), F32)], axis=0)
    total = jnp.sum(both.T, axis=0, keepdims=True)
    sums[...] = jnp.broadcast_to(total, (ALL_DEV, LANES))


def residual_kernel(gathered, modes, image_x, inverse_j, residual, whole, head, tail):
    total = jnp.sum(gathered[...], axis=0, keepdims=True)
    column = jnp.broadcast_to(total, (LANES, LANES)).T
    quotient = column[MODES:PAIR, :] / column[:MODES, :]
    for c in range(TILES):
        span = slice(c * LANES, (c + 1) * LANES)
        value = (image_x[:, span] - modes[:, span] * quotient) * inverse_j[:, span]
        residual[:, span] = value
        low = value.astype(BF16)
        whole[:, span] = low
        if c < HALO // LANES:
            head[:, span] = low
        if c >= TILES - HALO // LANES:
            at = (c - (TILES - HALO // LANES)) * LANES
            tail[:, at : at + LANES] = low


def inner_second_kernel(
    whole, other, tables, flipped, kinds, scales, rows, rows_o, weights,
    partial, coup, blocks, other_t,
):
    for b in range(NBR):
        blocks[b, :MODES] = whole[:, b * BS : (b + 1) * BS]
    for c in range(TILES):
        span = slice(c * LANES, (c + 1) * LANES)
        other_t[span, :MODES] = other[:, span].astype(F32).T
    coup[...] = jnp.zeros_like(coup)
    steps = (NBR - 4) // INNER
    slots = IFACE // steps

    def blocked(index, carry):
        beside = coupler(index * slots, slots, 5 * INNER - 1, rows, rows_o, weights, other_t, coup)
        for u in range(INNER):
            b = 2 + index * INNER + u
            total = block_sum(b, b, blocks, tables, flipped, kinds, scales, beside)
            partial[:, pl.ds(pl.multiple_of(b * BS, BS), BS)] = total[:MODES]
        return carry

    lax.fori_loop(0, steps, blocked, 0)


def outer_second_kernel(
    residual, whole, left, right, partial, coup, tables, flipped, kinds, scales,
    modes, prev, image_x, image_p, residual_out, packed, ends, image_e, gram, sem,
):
    copy = pltpu.make_async_copy(residual, residual_out, sem)
    copy.start()
    for b in range(2):
        span = slice(b * BS, (b + 1) * BS)
        ends[b, :MODES] = left[:, span]
        ends[10 + b, :MODES] = right[:, span]
    for at, b in ENDS:
        ends[at, :MODES] = whole[:, b * BS : (b + 1) * BS]
    gram[...] = jnp.zeros_like(gram)

    def blocked(index, carry):
        for u in range(2):
            b = index * (NBR - 2) + u
            total = block_sum(b, 2 + index * 6 + u, ends, tables, flipped, kinds, scales)
            at = (index * 2 + u) * BS
            image_e[:, pl.ds(pl.multiple_of(at, BS), BS)] = total[:MODES]
        return carry

    lax.fori_loop(0, 2, blocked, 0)

    def add(b, block_part):
        span = pl.ds(pl.multiple_of(b * 2 * BS, 2 * BS), 2 * BS)
        coupled = [
            coup[pl.ds(pl.multiple_of(b * 2 * BS + c * LANES, LANES), LANES), :].T[:MODES]
            for c in range(2 * BS // LANES)
        ]
        image = block_part + jnp.concatenate(coupled, axis=1)
        parts = [ref[:, span] for ref in (modes, residual, prev, image_x)]
        both = jnp.concatenate([*parts, image, image_p[:, span]], axis=0)
        high = both.astype(BF16)
        low = (both - high.astype(F32)).astype(BF16)
        gram[...] += lax.dot_general(
            jnp.concatenate([high, low], axis=0), high, (((1,), (1,)), ((), ())),
            preferred_element_type=F32,
        )

    def step(b, carry):
        add(b, partial[:, pl.ds(pl.multiple_of(b * 2 * BS, 2 * BS), 2 * BS)])
        return carry

    last = NBR // 2 - 1
    add(0, image_e[:, : 2 * BS])
    lax.fori_loop(1, last, step, 0)
    add(last, image_e[:, 2 * BS :])
    n = 3 * MODES
    pad = LANES - n
    zero_r = jnp.zeros((pad, n), F32)
    zero_c = jnp.zeros((LANES, pad), F32)

    def square(top, lane):
        value = gram[top : top + n, lane : lane + n]
        return jnp.concatenate([jnp.concatenate([value, zero_r], axis=0), zero_c], axis=1)

    cross_b = square(2 * n, 0)
    gram_b = square(0, 0) + cross_b + cross_b.T
    cross_a = square(0, n) + square(2 * n, n)
    raw = cross_a + square(3 * n, 0).T
    gram_a = raw + raw.T
    row = lax.broadcasted_iota(jnp.int32, (LANES, LANES), 0)
    col = lax.broadcasted_iota(jnp.int32, (LANES, LANES), 1)
    diagonal = jnp.sum(jnp.where(row == col, gram_a, 0.0), axis=0, keepdims=True)
    merged = jnp.where(row >= col, gram_b, gram_a)
    packed[...] = jnp.where(row == n, jnp.broadcast_to(diagonal, (LANES, LANES)), merged)
    copy.wait()


def lower_inverse(gram, count):
    group = 4
    tiles = count // 8
    sub = lax.broadcasted_iota(jnp.int32, (8, LANES), 0)
    lane = lax.broadcasted_iota(jnp.int32, (8, LANES), 1)
    left = [gram[8 * t : 8 * t + 8, :] for t in range(tiles)]
    right = [jnp.where(lane == sub + 8 * t, 1.0, 0.0).astype(F32) for t in range(tiles)]

    def spread(first):
        return [
            {
                t: jnp.broadcast_to(left[t][:, first + m : first + m + 1], (8, LANES))
                for t in range(first // 8, tiles)
            }
            for m in range(group)
        ]

    ahead = spread(0)
    for start in range(0, count, group):
        now = ahead
        ahead = spread(start + group) if start + group < count else []
        for k in range(group):
            pivot = start + k
            tile, r = divmod(pivot, 8)
            root = lax.rsqrt(now[k][tile][r : r + 1, :])
            factor = {t: now[k][t] * root for t in range(tile, tiles)}
            factor[tile] = jnp.where(sub > r, factor[tile], 0.0)
            for first, columns in ((start, now), (start + group, ahead)):
                for m, column in enumerate(columns):
                    at = first + m
                    if at <= pivot:
                        continue
                    own = factor[at // 8][at % 8 : at % 8 + 1, :]
                    for t in column:
                        column[t] = column[t] - factor[t] * own
            line_l = left[tile][r : r + 1, :] * root
            line_r = right[tile][r : r + 1, :] * root
            for t in range(tile, tiles):
                left[t] = left[t] - factor[t] * line_l
                right[t] = right[t] - factor[t] * line_r
            right[tile] = jnp.where(sub == r, line_r, right[tile])
    return right


def final_kernel(packed, modes, residual_in, prev, basis, projected, result, residual, sems):
    n = 3 * MODES
    load = pltpu.make_async_copy(residual_in, residual, sems.at[ROWS // WIDTH])
    load.start()
    row = lax.broadcasted_iota(jnp.int32, (LANES, LANES), 0)
    col = lax.broadcasted_iota(jnp.int32, (LANES, LANES), 1)
    merged = packed[...]
    flipped = merged.T
    inside = (row < n) & (col < n)
    ndof = jnp.float32(2.0 * 64 * ROWS)
    gram_b = jnp.where(inside, jnp.where(row >= col, merged, flipped) / ndof, 0.0)
    diagonal = jnp.broadcast_to(merged[n : n + 1, :], (LANES, LANES))
    gram_a = jnp.where(row < col, merged, flipped)
    gram_a = jnp.where(row == col, diagonal, gram_a) / (2.0 * ndof)
    gram_a = jnp.where(inside, gram_a, 0.0)
    factors = jnp.concatenate(lower_inverse(gram_b, n), axis=0)
    half = lax.dot_general(
        factors, gram_a, (((1,), (0,)), ((), ())),
        precision=lax.Precision.HIGHEST, preferred_element_type=F32,
    )
    whole = lax.dot_general(
        half, factors, (((1,), (1,)), ((), ())),
        precision=lax.Precision.HIGHEST, preferred_element_type=F32,
    )
    projected[...] = whole
    factors = factors[:, :n]
    high = factors.astype(BF16)
    low = (factors - high.astype(F32)).astype(BF16)
    top = jnp.concatenate([high, high], axis=1)
    dims = (((1,), (0,)), ((), ()))
    load.wait()
    stores = []
    for index in range(ROWS // WIDTH):
        span = pl.ds(index * WIDTH, WIDTH)
        part = jnp.concatenate([modes[:, span], residual[:, span], prev[:, span]], axis=0)
        part_h = part.astype(BF16)
        part_l = (part - part_h.astype(F32)).astype(BF16)
        stacked = jnp.concatenate([part_h, part_l], axis=0)
        result[:, span] = lax.dot_general(
            top, stacked, dims, preferred_element_type=F32
        ) + lax.dot_general(low, part_h, dims, preferred_element_type=F32)
        store = pltpu.make_async_copy(
            result.at[:, span], basis.at[:, span], sems.at[index]
        )
        store.start()
        stores.append(store)
    for store in stores:
        store.wait()


def shards(modes, previous, kinds, scales, tables, wet_rows, wet_counts, coupling):
    modes = modes[0]
    prev = previous[0]
    kinds = kinds[0].reshape(3 * NBLK)
    scales = scales[0].reshape(3 * NBLK)
    tables = tables[0].reshape(3 * NTYPE, BS, BS)
    rows = wet_rows[0]
    modes, prev, whole, head, tail, weights, rows = rounded_parts(
        modes, prev, coupling, rows, wet_counts
    )
    weights = weights.reshape(IFACE)
    rows_o = swap_field(rows).reshape(IFACE)
    rows = rows.reshape(IFACE)
    other = swap_field(whole)
    left = from_left(tail)
    right = from_right(head)
    coupling_args = (rows, rows_o, weights)
    plane = shape(MODES, ROWS)
    rows_by_lanes = shape(ROWS, LANES)
    end = shape(PAIR, HALO)
    partial_x, partial_p, coup, tables, flipped = pl.pallas_call(
        inner_kernel,
        out_shape=(
            plane, plane, rows_by_lanes,
            shape(3 * NTYPE, BS, BS, kind=BF16), shape(2 * NTYPE, BS, BS, kind=BF16),
        ),
        in_specs=[VMEM] * 3 + [HBM] + [SMEM] * 5,
        out_specs=[VMEM] * 5,
        scratch_shapes=[
            pltpu.VMEM((NBR, PAIR, BS), BF16),
            pltpu.VMEM((ROWS, LANES), F32),
            pltpu.SemaphoreType.DMA((3,)),
        ],
        compiler_params=params(10),
        name="inner",
    )(modes, prev, other, in_hbm(tables), kinds, scales, *coupling_args)
    image_x, image_p, inverse_j, sums = pl.pallas_call(
        outer_kernel,
        out_shape=(plane, plane, shape(1, ROWS), shape(ALL_DEV, LANES)),
        in_specs=[VMEM] * 9 + [SMEM] * 2,
        out_specs=[VMEM] * 4,
        scratch_shapes=[pltpu.VMEM((12, PAIR, BS), BF16)],
        compiler_params=params(6),
        name="outer",
    )(modes, prev, left, right, partial_x, partial_p, coup, tables, flipped, kinds, scales)
    gathered = exchange(sums)
    end = shape(MODES, HALO, kind=BF16)
    residual, whole, head, tail = pl.pallas_call(
        residual_kernel,
        out_shape=(plane, shape(MODES, ROWS, kind=BF16), end, end),
        in_specs=[VMEM] * 4,
        out_specs=[VMEM] * 4,
        compiler_params=params(6),
        name="residual",
    )(gathered, modes, image_x, inverse_j)
    other = swap_field(whole)
    left = from_left(tail)
    right = from_right(head)
    partial, coup = pl.pallas_call(
        inner_second_kernel,
        out_shape=(plane, rows_by_lanes),
        in_specs=[VMEM] * 4 + [SMEM] * 5,
        out_specs=[VMEM] * 2,
        scratch_shapes=[
            pltpu.VMEM((NBR, SINGLE, BS), BF16),
            pltpu.VMEM((ROWS, LANES), F32),
        ],
        compiler_params=params(10),
        name="inner_second",
    )(whole, other, tables, flipped, kinds, scales, *coupling_args)
    residual, packed = pl.pallas_call(
        outer_second_kernel,
        out_shape=(pltpu.HBM((MODES, ROWS), F32), shape(LANES, LANES)),
        in_specs=[VMEM] * 8 + [SMEM] * 2 + [VMEM] * 4,
        out_specs=[HBM, VMEM],
        scratch_shapes=[
            pltpu.VMEM((12, SINGLE, BS), BF16),
            pltpu.VMEM((MODES, 4 * BS), F32),
            pltpu.VMEM((12 * MODES, 6 * MODES), F32),
            pltpu.SemaphoreType.DMA(()),
        ],
        compiler_params=params(10),
        name="outer_second",
    )(
        residual, whole, left, right, partial, coup, tables, flipped, kinds, scales,
        modes, prev, image_x, image_p,
    )
    part = jnp.sum(exchange(packed), axis=0, keepdims=True)
    packed = exchange(jnp.broadcast_to(part, (ALL_DEV, LANES)))
    n = 3 * MODES
    basis, projected = pl.pallas_call(
        final_kernel,
        out_shape=(pltpu.HBM((n, ROWS), F32), shape(n, n)),
        in_specs=[VMEM, VMEM, HBM, VMEM],
        out_specs=[HBM, VMEM],
        scratch_shapes=[
            pltpu.VMEM((n, ROWS), F32),
            pltpu.VMEM((MODES, ROWS), F32),
            pltpu.SemaphoreType.DMA((ROWS // WIDTH + 1,)),
        ],
        compiler_params=params(14),
        name="final",
    )(packed, modes, in_hbm(residual), prev)
    return (basis[None], projected)


def solution(mesh):
    finer = Mesh(
        mesh.devices.reshape(mesh.shape["field"], 4, 4, 4), ("field", "dom_0", "dom_1", "dom_2")
    )
    placed = (
        P("field", None, DOM),
        P("field", None, DOM),
        P("field", None, None),
        P("field", None, None),
        P("field", None, None, None, None),
        P("field", DOM),
        P(DOM),
        P(DOM),
    )
    return jax.shard_map(
        shards, mesh=finer, in_specs=placed, out_specs=(P("field", None, DOM), P()), check_vma=False
    )
```

```python
import jax
import jax.numpy as jnp
from jax import lax
from jax.experimental import pallas as pl
from jax.experimental.pallas import tpu as pltpu
from jax.sharding import Mesh
from jax.sharding import PartitionSpec as P


BS = 512
NTYPE = 4
NBR = 16
NBLK = 1024
ROWS = NBR * BS
HALO = 2 * BS
MODES = 40
IFACE = 3072
LANES = 128
TILES = ROWS // LANES
DOM = ("dom_0", "dom_1", "dom_2")
FIELD_DOM = ("field", "dom_0", "dom_1", "dom_2")
ALL_DEV = 128
F32 = jnp.float32
BF16 = jnp.bfloat16

VMEM = pl.BlockSpec(memory_space=pltpu.VMEM)
SMEM = pl.BlockSpec(memory_space=pltpu.SMEM)
HBM = pl.BlockSpec(memory_space=pltpu.HBM)
PAIR = 2 * MODES
SINGLE = 48
INNER = 6
ENDS = ((2, 0), (3, 1), (4, 2), (5, 3), (6, 12), (7, 13), (8, 14), (9, 15))
WIDTH = 1024

OPS = ((0, 0, 0, 0), (1, -1, -1, 0), (2, -2, -2, 0), (1, 1, 0, 1), (2, 2, 0, 1))


def params(mib):
    return pltpu.CompilerParams(vmem_limit_bytes=mib << 20)


def shape(*dims, kind=F32):
    return jax.ShapeDtypeStruct(dims, kind)


def domain_index():
    return (lax.axis_index(DOM[0]) * 4 + lax.axis_index(DOM[1])) * 4 + lax.axis_index(DOM[2])


def in_hbm(value):
    return pltpu.with_memory_space_constraint(value, pltpu.HBM)


def swap_field(value):
    return lax.ppermute(value, "field", [(0, 1), (1, 0)])


def is_even():
    return lax.rem(lax.axis_index(DOM[2]), 2) == 0


def pick(condition, one, two):
    return jnp.where(condition, one, two)


def swap_pairs(value, first):
    pairs = [(i, i + 1) for i in range(first, 63, 2)]
    return lax.ppermute(value, DOM, pairs + [(j, i) for i, j in pairs])


def exchange(rows):
    return lax.all_to_all(rows, FIELD_DOM, 0, 0, tiled=True)


def round_kernel(
    modes, prev, coupling, rows, counts,
    modes_v, prev_v, whole, to_near, to_far, weights, rows_v, sems,
):
    pairs = ((modes, modes_v), (prev, prev_v), (coupling, weights), (rows, rows_v))
    loads = [
        pltpu.make_async_copy(source, target, sems.at[index])
        for index, (source, target) in enumerate(pairs)
    ]
    for load in loads:
        load.start()
    slot = lax.broadcasted_iota(jnp.int32, weights.shape, 0) * LANES + lax.broadcasted_iota(
        jnp.int32, weights.shape, 1
    )
    for load in loads:
        load.wait()
    weights[...] = jnp.where(slot < counts[0], weights[...], 0.0)
    rounded = jnp.concatenate([modes_v[...], prev_v[...]], axis=0).astype(BF16)
    whole[...] = rounded
    even = is_even()
    head, tail = rounded[:, :HALO], rounded[:, ROWS - HALO :]
    to_near[...] = pick(even, tail, head)
    to_far[...] = pick(even, head, tail)


def rounded_parts(modes, prev, coupling, rows, counts):
    plane = shape(MODES, ROWS)
    end = shape(PAIR, HALO, kind=BF16)
    slots = shape(IFACE // LANES, LANES)
    return pl.pallas_call(
        round_kernel,
        out_shape=(plane, plane, shape(PAIR, ROWS, kind=BF16), end, end, slots,
                   shape(IFACE // LANES, LANES, kind=jnp.int32)),
        in_specs=[HBM] * 4 + [SMEM],
        out_specs=[VMEM] * 7,
        scratch_shapes=[pltpu.SemaphoreType.DMA((4,))],
        compiler_params=params(12),
        name="rounded",
    )(
        *map(in_hbm, (modes, prev, coupling.reshape(slots.shape), rows.reshape(slots.shape))),
        counts,
    )


def fetch(sources, targets, sems):
    copies = [
        pltpu.make_async_copy(source, target, sems.at[index])
        for index, (source, target) in enumerate(zip(sources, targets))
    ]
    for copy in copies:
        copy.start()
    return copies


def scalar_scratch(coupled):
    kinds = [jnp.int32, F32] + [jnp.int32, jnp.int32, F32] * coupled
    return [pltpu.SMEM((IFACE,), kind) for kind in kinds] + [
        pltpu.SemaphoreType.DMA((len(kinds),))
    ]


def block_sum(b, at, blocks, tables, flipped, kinds, scales, beside=None):
    first = domain_index() * NBR
    total = None
    for index, (offset, shift, owner, flip) in enumerate(OPS):
        block = offset * NBLK + jnp.maximum(first + b + owner, 0)
        kind = kinds[block]
        if flip:
            table = flipped[(offset - 1) * NTYPE + kind]
        else:
            table = tables[offset * NTYPE + kind]
        product = jnp.dot(blocks[at + shift], table, preferred_element_type=F32)
        if beside is not None:
            beside(index, product[0, 0])
        product = scales[block] * product
        total = product if total is None else total + product
    return total


def coupler(base, total, dots, rows, rows_o, weights, other_t, coup):
    cuts = [total * index // dots for index in range(dots + 1)]
    taken = []

    def beside(_, value):
        if len(taken) == dots:
            return
        late = jnp.where(value == value, 0, 1)
        cut, share = cuts[len(taken)], cuts[len(taken) + 1] - cuts[len(taken)]
        start = jnp.minimum(base + cut + late, IFACE - share)
        taken.append(start)
        for v in range(share):
            slot = start + v
            coup[pl.ds(rows[slot], 1), :] = other_t[pl.ds(rows_o[slot], 1), :] * weights[slot]

    return beside


def inner_kernel(
    modes, prev, other, tables_in, *refs
):
    scalars, refs = refs[:5], refs[5:]
    partial_x, partial_p, coup, tables, flipped, blocks, other_t, sems = refs[:8]
    kinds, scales, rows, rows_o, weights, scalar_sems = refs[8:]
    fetched = fetch(scalars, (kinds, scales, rows, rows_o, weights), scalar_sems)
    loads = [
        pltpu.make_async_copy(
            tables_in.at[pl.ds(offset * NTYPE, NTYPE)],
            tables.at[pl.ds(offset * NTYPE, NTYPE)],
            sems.at[offset],
        )
        for offset in range(3)
    ]
    for offset in (1, 2, 0):
        loads[offset].start()
    for b in range(NBR):
        span = slice(b * BS, (b + 1) * BS)
        blocks[b] = jnp.concatenate([modes[:, span], prev[:, span]], axis=0).astype(BF16)
    for c in range(TILES):
        span = slice(c * LANES, (c + 1) * LANES)
        other_t[span, :PAIR] = other[:, span].astype(F32).T
    coup[...] = jnp.zeros_like(coup)
    for offset in (1, 2):
        loads[offset].wait()
        for index in range(NTYPE):
            flipped[(offset - 1) * NTYPE + index] = tables[offset * NTYPE + index].T
    loads[0].wait()
    for copy in fetched:
        copy.wait()
    steps = (NBR - 4) // INNER
    slots = IFACE // steps

    def step(index, carry):
        beside = coupler(index * slots, slots, 5 * INNER - 1, rows, rows_o, weights, other_t, coup)
        for u in range(INNER):
            b = 2 + index * INNER + u
            total = block_sum(b, b, blocks, tables, flipped, kinds, scales, beside)
            span = pl.ds(pl.multiple_of(b * BS, BS), BS)
            partial_x[:, span] = total[:MODES]
            partial_p[:, span] = total[MODES:]
        return carry

    lax.fori_loop(0, steps, step, 0)


def outer_kernel(
    modes, prev, near, far, partial_x, partial_p, coup, tables, flipped, kinds_in, scales_in,
    image_x, image_p, inverse_j, sums, ends, kinds, scales, scalar_sems,
):
    fetched = fetch((kinds_in, scales_in), (kinds, scales), scalar_sems)
    first = domain_index() * NBR
    even = is_even()
    for b in range(2):
        span = slice(b * BS, (b + 1) * BS)
        ends[b] = pick(even, far[:, span], near[:, span])
        ends[10 + b] = pick(even, near[:, span], far[:, span])
    for at, b in ENDS:
        span = slice(b * BS, (b + 1) * BS)
        ends[at] = jnp.concatenate([modes[:, span], prev[:, span]], axis=0).astype(BF16)

    for copy in fetched:
        copy.wait()

    def step(index, carry):
        for u in range(2):
            b = index * (NBR - 2) + u
            total = block_sum(b, 2 + index * 6 + u, ends, tables, flipped, kinds, scales)
            span = pl.ds(pl.multiple_of(b * BS, BS), BS)
            image_x[:, span] = total[:MODES]
            image_p[:, span] = total[MODES:]
        return carry

    lax.fori_loop(0, 2, step, 0)
    on_diagonal = lax.broadcasted_iota(jnp.int32, (LANES, LANES), 0) == lax.broadcasted_iota(
        jnp.int32, (LANES, LANES), 1
    )
    lines = []
    for part in range(BS // LANES):
        span = slice(part * LANES, (part + 1) * LANES)
        lines.append(
            [
                jnp.sum(
                    jnp.where(on_diagonal, tables[kind, span, span].astype(F32), 0.0),
                    axis=0, keepdims=True,
                )
                for kind in range(NTYPE)
            ]
        )
    squares = jnp.zeros((MODES, LANES), F32)
    crossed = jnp.zeros((MODES, LANES), F32)
    for c in range(TILES):
        b, part = divmod(c, BS // LANES)
        span = slice(c * LANES, (c + 1) * LANES)
        coupled = coup[span, :].T
        source_x, source_p = (partial_x, partial_p) if 2 <= b < NBR - 2 else (image_x, image_p)
        value = source_x[:, span] + coupled[:MODES]
        image_x[:, span] = value
        image_p[:, span] = source_p[:, span] + coupled[MODES:PAIR]
        own = modes[:, span]
        squares += own * own
        crossed += own * value
        kind = kinds[first + b]
        line = lines[part][0]
        for other_kind in range(1, NTYPE):
            line = jnp.where(kind == other_kind, lines[part][other_kind], line)
        inverse_j[:, span] = 1.0 / (scales[first + b] * line)
    both = jnp.concatenate([squares, crossed, jnp.zeros((LANES - PAIR, LANES), F32)], axis=0)
    total = jnp.sum(both.T, axis=0, keepdims=True)
    sums[...] = jnp.broadcast_to(total, (ALL_DEV, LANES))


def residual_kernel(gathered, modes, image_x, inverse_j, residual, whole, to_near, to_far):
    total = jnp.sum(gathered[...], axis=0, keepdims=True)
    column = jnp.broadcast_to(total, (LANES, LANES)).T
    quotient = column[MODES:PAIR, :] / column[:MODES, :]
    for c in range(TILES):
        span = slice(c * LANES, (c + 1) * LANES)
        value = (image_x[:, span] - modes[:, span] * quotient) * inverse_j[:, span]
        residual[:, span] = value
        whole[:, span] = value.astype(BF16)
    even = is_even()
    head, tail = whole[:, :HALO], whole[:, ROWS - HALO :]
    to_near[...] = pick(even, tail, head)
    to_far[...] = pick(even, head, tail)


def inner_second_kernel(
    whole, other, tables, flipped, *refs
):
    scalars, refs = refs[:5], refs[5:]
    partial, coup, blocks, other_t, kinds, scales, rows, rows_o, weights, scalar_sems = refs
    fetched = fetch(scalars, (kinds, scales, rows, rows_o, weights), scalar_sems)
    for b in range(NBR):
        blocks[b, :MODES] = whole[:, b * BS : (b + 1) * BS]
    for c in range(TILES):
        span = slice(c * LANES, (c + 1) * LANES)
        other_t[span, :MODES] = other[:, span].astype(F32).T
    coup[...] = jnp.zeros_like(coup)
    for copy in fetched:
        copy.wait()
    steps = (NBR - 4) // INNER
    slots = IFACE // steps

    def blocked(index, carry):
        beside = coupler(index * slots, slots, 5 * INNER - 1, rows, rows_o, weights, other_t, coup)
        for u in range(INNER):
            b = 2 + index * INNER + u
            total = block_sum(b, b, blocks, tables, flipped, kinds, scales, beside)
            partial[:, pl.ds(pl.multiple_of(b * BS, BS), BS)] = total[:MODES]
        return carry

    lax.fori_loop(0, steps, blocked, 0)


def outer_second_kernel(
    residual, whole, near, far, partial, coup, tables, flipped, kinds_in, scales_in,
    modes, prev, image_x, image_p, residual_out, packed, ends, image_e, gram, sem,
    kinds, scales, scalar_sems,
):
    fetched = fetch((kinds_in, scales_in), (kinds, scales), scalar_sems)
    even = is_even()
    stored = pltpu.make_async_copy(residual, residual_out, sem)
    stored.start()
    for b in range(2):
        span = slice(b * BS, (b + 1) * BS)
        ends[b, :MODES] = pick(even, far[:, span], near[:, span])
        ends[10 + b, :MODES] = pick(even, near[:, span], far[:, span])
    for at, b in ENDS:
        ends[at, :MODES] = whole[:, b * BS : (b + 1) * BS]
    gram[...] = jnp.zeros_like(gram)

    for copy in fetched:
        copy.wait()

    def blocked(index, carry):
        for u in range(2):
            b = index * (NBR - 2) + u
            total = block_sum(b, 2 + index * 6 + u, ends, tables, flipped, kinds, scales)
            at = (index * 2 + u) * BS
            image_e[:, pl.ds(pl.multiple_of(at, BS), BS)] = total[:MODES]
        return carry

    lax.fori_loop(0, 2, blocked, 0)

    def add(b, block_part):
        span = pl.ds(pl.multiple_of(b * 2 * BS, 2 * BS), 2 * BS)
        coupled = [
            coup[pl.ds(pl.multiple_of(b * 2 * BS + c * LANES, LANES), LANES), :].T[:MODES]
            for c in range(2 * BS // LANES)
        ]
        image = block_part + jnp.concatenate(coupled, axis=1)
        parts = [ref[:, span] for ref in (modes, residual, prev, image_x)]
        both = jnp.concatenate([*parts, image, image_p[:, span]], axis=0)
        high = both.astype(BF16)
        low = (both - high.astype(F32)).astype(BF16)
        gram[...] += lax.dot_general(
            jnp.concatenate([high, low], axis=0), high, (((1,), (1,)), ((), ())),
            preferred_element_type=F32,
        )

    def step(b, carry):
        add(b, partial[:, pl.ds(pl.multiple_of(b * 2 * BS, 2 * BS), 2 * BS)])
        return carry

    last = NBR // 2 - 1
    add(0, image_e[:, : 2 * BS])
    lax.fori_loop(1, last, step, 0)
    add(last, image_e[:, 2 * BS :])
    n = 3 * MODES
    pad = LANES - n
    zero_r = jnp.zeros((pad, n), F32)
    zero_c = jnp.zeros((LANES, pad), F32)

    def square(top, lane):
        value = gram[top : top + n, lane : lane + n]
        return jnp.concatenate([jnp.concatenate([value, zero_r], axis=0), zero_c], axis=1)

    cross_b = square(2 * n, 0)
    gram_b = square(0, 0) + cross_b + cross_b.T
    cross_a = square(0, n) + square(2 * n, n)
    raw = cross_a + square(3 * n, 0).T
    gram_a = raw + raw.T
    row = lax.broadcasted_iota(jnp.int32, (LANES, LANES), 0)
    col = lax.broadcasted_iota(jnp.int32, (LANES, LANES), 1)
    diagonal = jnp.sum(jnp.where(row == col, gram_a, 0.0), axis=0, keepdims=True)
    merged = jnp.where(row >= col, gram_b, gram_a)
    packed[...] = jnp.where(row == n, jnp.broadcast_to(diagonal, (LANES, LANES)), merged)
    stored.wait()


def lower_inverse(gram, count):
    group = 4
    tiles = count // 8
    sub = lax.broadcasted_iota(jnp.int32, (8, LANES), 0)
    lane = lax.broadcasted_iota(jnp.int32, (8, LANES), 1)
    left = [gram[8 * t : 8 * t + 8, :] for t in range(tiles)]
    right = [jnp.where(lane == sub + 8 * t, 1.0, 0.0).astype(F32) for t in range(tiles)]

    def spread(first):
        return [
            {
                t: jnp.broadcast_to(left[t][:, first + m : first + m + 1], (8, LANES))
                for t in range(first // 8, tiles)
            }
            for m in range(group)
        ]

    ahead = spread(0)
    for start in range(0, count, group):
        now = ahead
        ahead = spread(start + group) if start + group < count else []
        for k in range(group):
            pivot = start + k
            tile, r = divmod(pivot, 8)
            root = lax.rsqrt(now[k][tile][r : r + 1, :])
            factor = {t: now[k][t] * root for t in range(tile, tiles)}
            factor[tile] = jnp.where(sub > r, factor[tile], 0.0)
            for first, columns in ((start, now), (start + group, ahead)):
                for m, column in enumerate(columns):
                    at = first + m
                    if at <= pivot:
                        continue
                    own = factor[at // 8][at % 8 : at % 8 + 1, :]
                    for t in column:
                        column[t] = column[t] - factor[t] * own
            line_l = left[tile][r : r + 1, :] * root
            line_r = right[tile][r : r + 1, :] * root
            for t in range(tile, tiles):
                left[t] = left[t] - factor[t] * line_l
                right[t] = right[t] - factor[t] * line_r
            right[tile] = jnp.where(sub == r, line_r, right[tile])
    return right


def final_kernel(packed, modes, residual_in, prev, basis, projected, result, residual, sems):
    n = 3 * MODES
    load = pltpu.make_async_copy(residual_in, residual, sems.at[ROWS // WIDTH])
    load.start()
    row = lax.broadcasted_iota(jnp.int32, (LANES, LANES), 0)
    col = lax.broadcasted_iota(jnp.int32, (LANES, LANES), 1)
    merged = packed[...]
    flipped = merged.T
    inside = (row < n) & (col < n)
    ndof = jnp.float32(2.0 * 64 * ROWS)
    gram_b = jnp.where(inside, jnp.where(row >= col, merged, flipped) / ndof, 0.0)
    diagonal = jnp.broadcast_to(merged[n : n + 1, :], (LANES, LANES))
    gram_a = jnp.where(row < col, merged, flipped)
    gram_a = jnp.where(row == col, diagonal, gram_a) / (2.0 * ndof)
    gram_a = jnp.where(inside, gram_a, 0.0)
    factors = jnp.concatenate(lower_inverse(gram_b, n), axis=0)
    square = factors[:, :n]
    high = square.astype(BF16)
    low = (square - high.astype(F32)).astype(BF16)
    top = jnp.concatenate([high, high], axis=1)
    dims = (((1,), (0,)), ((), ()))
    load.wait()
    stores = []
    for index in range(ROWS // WIDTH):
        span = pl.ds(index * WIDTH, WIDTH)
        part = jnp.concatenate([modes[:, span], residual[:, span], prev[:, span]], axis=0)
        part_h = part.astype(BF16)
        part_l = (part - part_h.astype(F32)).astype(BF16)
        stacked = jnp.concatenate([part_h, part_l], axis=0)
        result[:, span] = lax.dot_general(
            top, stacked, dims, preferred_element_type=F32
        ) + lax.dot_general(low, part_h, dims, preferred_element_type=F32)
        store = pltpu.make_async_copy(
            result.at[:, span], basis.at[:, span], sems.at[index]
        )
        store.start()
        stores.append(store)
    half = lax.dot_general(
        factors, gram_a, (((1,), (0,)), ((), ())),
        precision=lax.Precision.HIGHEST, preferred_element_type=F32,
    )
    whole = lax.dot_general(
        half, factors, (((1,), (1,)), ((), ())),
        precision=lax.Precision.HIGHEST, preferred_element_type=F32,
    )
    projected[...] = whole
    for store in stores:
        store.wait()


def shards(modes, previous, kinds, scales, tables, wet_rows, wet_counts, coupling):
    modes = modes[0]
    prev = previous[0]
    kinds = kinds[0].reshape(3 * NBLK)
    scales = scales[0].reshape(3 * NBLK)
    tables = tables[0].reshape(3 * NTYPE, BS, BS)
    rows = wet_rows[0]
    modes, prev, whole, to_near, to_far, weights, rows = rounded_parts(
        modes, prev, coupling, rows, wet_counts
    )
    weights = weights.reshape(IFACE)
    rows_o = swap_field(rows).reshape(IFACE)
    rows = rows.reshape(IFACE)
    other = swap_field(whole)
    near = swap_pairs(to_near, 0)
    far = swap_pairs(to_far, 1)
    coupling_args = (rows, rows_o, weights)
    plane = shape(MODES, ROWS)
    rows_by_lanes = shape(ROWS, LANES)
    end = shape(PAIR, HALO)
    partial_x, partial_p, coup, tables, flipped = pl.pallas_call(
        inner_kernel,
        out_shape=(
            plane, plane, rows_by_lanes,
            shape(3 * NTYPE, BS, BS, kind=BF16), shape(2 * NTYPE, BS, BS, kind=BF16),
        ),
        in_specs=[VMEM] * 3 + [HBM] + [VMEM] * 5,
        out_specs=[VMEM] * 5,
        scratch_shapes=[
            pltpu.VMEM((NBR, PAIR, BS), BF16),
            pltpu.VMEM((ROWS, LANES), F32),
            pltpu.SemaphoreType.DMA((3,)),
            *scalar_scratch(True),
        ],
        compiler_params=params(10),
        name="inner",
    )(modes, prev, other, in_hbm(tables), kinds, scales, *coupling_args)
    image_x, image_p, inverse_j, sums = pl.pallas_call(
        outer_kernel,
        out_shape=(plane, plane, shape(1, ROWS), shape(ALL_DEV, LANES)),
        in_specs=[VMEM] * 11,
        out_specs=[VMEM] * 4,
        scratch_shapes=[pltpu.VMEM((12, PAIR, BS), BF16), *scalar_scratch(False)],
        compiler_params=params(6),
        name="outer",
    )(modes, prev, near, far, partial_x, partial_p, coup, tables, flipped, kinds, scales)
    gathered = exchange(sums)
    end = shape(MODES, HALO, kind=BF16)
    residual, whole, to_near, to_far = pl.pallas_call(
        residual_kernel,
        out_shape=(plane, shape(MODES, ROWS, kind=BF16), end, end),
        in_specs=[VMEM] * 4,
        out_specs=[VMEM] * 4,
        compiler_params=params(6),
        name="residual",
    )(gathered, modes, image_x, inverse_j)
    other = swap_field(whole)
    near = swap_pairs(to_near, 0)
    far = swap_pairs(to_far, 1)
    partial, coup = pl.pallas_call(
        inner_second_kernel,
        out_shape=(plane, rows_by_lanes),
        in_specs=[VMEM] * 9,
        out_specs=[VMEM] * 2,
        scratch_shapes=[
            pltpu.VMEM((NBR, SINGLE, BS), BF16),
            pltpu.VMEM((ROWS, LANES), F32),
            *scalar_scratch(True),
        ],
        compiler_params=params(10),
        name="inner_second",
    )(whole, other, tables, flipped, kinds, scales, *coupling_args)
    residual, packed = pl.pallas_call(
        outer_second_kernel,
        out_shape=(pltpu.HBM((MODES, ROWS), F32), shape(LANES, LANES)),
        in_specs=[VMEM] * 14,
        out_specs=[HBM, VMEM],
        scratch_shapes=[
            pltpu.VMEM((12, SINGLE, BS), BF16),
            pltpu.VMEM((MODES, 4 * BS), F32),
            pltpu.VMEM((12 * MODES, 6 * MODES), F32),
            pltpu.SemaphoreType.DMA(()),
            *scalar_scratch(False),
        ],
        compiler_params=params(10),
        name="outer_second",
    )(
        residual, whole, near, far, partial, coup, tables, flipped, kinds, scales,
        modes, prev, image_x, image_p,
    )
    part = jnp.sum(exchange(packed), axis=0, keepdims=True)
    packed = exchange(jnp.broadcast_to(part, (ALL_DEV, LANES)))
    n = 3 * MODES
    basis, projected = pl.pallas_call(
        final_kernel,
        out_shape=(pltpu.HBM((n, ROWS), F32), shape(n, n)),
        in_specs=[VMEM, VMEM, HBM, VMEM],
        out_specs=[HBM, VMEM],
        scratch_shapes=[
            pltpu.VMEM((n, ROWS), F32),
            pltpu.VMEM((MODES, ROWS), F32),
            pltpu.SemaphoreType.DMA((ROWS // WIDTH + 1,)),
        ],
        compiler_params=params(14),
        name="final",
    )(packed, modes, in_hbm(residual), prev)
    return (basis[None], projected)


def solution(mesh):
    finer = Mesh(
        mesh.devices.reshape(mesh.shape["field"], 4, 4, 4), ("field", "dom_0", "dom_1", "dom_2")
    )
    placed = (
        P("field", None, DOM),
        P("field", None, DOM),
        P("field", None, None),
        P("field", None, None),
        P("field", None, None, None, None),
        P("field", DOM),
        P(DOM),
        P(DOM),
    )
    return jax.shard_map(
        shards, mesh=finer, in_specs=placed, out_specs=(P("field", None, DOM), P()), check_vma=False
    )
```

```python
import jax
import jax.numpy as jnp
from jax import lax
from jax.experimental import pallas as pl
from jax.experimental.pallas import tpu as pltpu
from jax.sharding import Mesh
from jax.sharding import PartitionSpec as P


BS = 512
NTYPE = 4
NBR = 16
NBLK = 1024
ROWS = NBR * BS
HALO = 2 * BS
MODES = 40
IFACE = 3072
LANES = 128
TILES = ROWS // LANES
DOM = ("dom_0", "dom_1", "dom_2")
FIELD_DOM = ("field", "dom_0", "dom_1", "dom_2")
ALL_DEV = 128
F32 = jnp.float32
BF16 = jnp.bfloat16

VMEM = pl.BlockSpec(memory_space=pltpu.VMEM)
SMEM = pl.BlockSpec(memory_space=pltpu.SMEM)
HBM = pl.BlockSpec(memory_space=pltpu.HBM)
PAIR = 2 * MODES
SINGLE = 48
INNER = 6
ENDS = ((2, 0), (3, 1), (4, 2), (5, 3), (6, 12), (7, 13), (8, 14), (9, 15))
WIDTH = 1024

OPS = ((0, 0, 0, 0), (1, -1, -1, 0), (2, -2, -2, 0), (1, 1, 0, 1), (2, 2, 0, 1))


def params(mib):
    return pltpu.CompilerParams(vmem_limit_bytes=mib << 20)


def shape(*dims, kind=F32):
    return jax.ShapeDtypeStruct(dims, kind)


def domain_index():
    return (lax.axis_index(DOM[0]) * 4 + lax.axis_index(DOM[1])) * 4 + lax.axis_index(DOM[2])


def in_hbm(value):
    return pltpu.with_memory_space_constraint(value, pltpu.HBM)


def swap_field(value):
    return lax.ppermute(value, "field", [(0, 1), (1, 0)])


def is_even():
    return lax.rem(lax.axis_index(DOM[2]), 2) == 0


def pick(condition, one, two):
    return jnp.where(condition, one, two)


def swap_pairs(value, first):
    pairs = [(i, i + 1) for i in range(first, 63, 2)]
    return lax.ppermute(value, DOM, pairs + [(j, i) for i, j in pairs])


def exchange(rows):
    return lax.all_to_all(rows, FIELD_DOM, 0, 0, tiled=True)


def round_kernel(
    modes, prev, coupling, rows, counts,
    modes_v, prev_v, whole, to_near, to_far, weights, rows_v, sems,
):
    pairs = ((modes, modes_v), (prev, prev_v), (coupling, weights), (rows, rows_v))
    loads = [
        pltpu.make_async_copy(source, target, sems.at[index])
        for index, (source, target) in enumerate(pairs)
    ]
    for load in loads:
        load.start()
    slot = lax.broadcasted_iota(jnp.int32, weights.shape, 0) * LANES + lax.broadcasted_iota(
        jnp.int32, weights.shape, 1
    )
    for load in loads:
        load.wait()
    weights[...] = jnp.where(slot < counts[0], weights[...], 0.0)
    rounded = jnp.concatenate([modes_v[...], prev_v[...]], axis=0).astype(BF16)
    whole[...] = rounded
    even = is_even()
    head, tail = rounded[:, :HALO], rounded[:, ROWS - HALO :]
    to_near[...] = pick(even, tail, head)
    to_far[...] = pick(even, head, tail)


def rounded_parts(modes, prev, coupling, rows, counts):
    plane = shape(MODES, ROWS)
    end = shape(PAIR, HALO, kind=BF16)
    slots = shape(IFACE // LANES, LANES)
    return pl.pallas_call(
        round_kernel,
        out_shape=(plane, plane, shape(PAIR, ROWS, kind=BF16), end, end, slots,
                   shape(IFACE // LANES, LANES, kind=jnp.int32)),
        in_specs=[HBM] * 4 + [SMEM],
        out_specs=[VMEM] * 7,
        scratch_shapes=[pltpu.SemaphoreType.DMA((4,))],
        compiler_params=params(12),
        name="rounded",
    )(
        *map(in_hbm, (modes, prev, coupling.reshape(slots.shape), rows.reshape(slots.shape))),
        counts,
    )


def fetch(sources, targets, sems):
    copies = [
        pltpu.make_async_copy(source, target, sems.at[index])
        for index, (source, target) in enumerate(zip(sources, targets))
    ]
    for copy in copies:
        copy.start()
    return copies


def scalar_scratch(coupled):
    kinds = [jnp.int32, F32] + [jnp.int32, jnp.int32, F32] * coupled
    return [pltpu.SMEM((IFACE,), kind) for kind in kinds] + [
        pltpu.SemaphoreType.DMA((len(kinds),))
    ]


def block_sum(b, at, blocks, tables, flipped, kinds, scales, beside=None):
    first = domain_index() * NBR
    total = None
    for index, (offset, shift, owner, flip) in enumerate(OPS):
        block = offset * NBLK + jnp.maximum(first + b + owner, 0)
        kind = kinds[block]
        if flip:
            table = flipped[(offset - 1) * NTYPE + kind]
        else:
            table = tables[offset * NTYPE + kind]
        product = jnp.dot(blocks[at + shift], table, preferred_element_type=F32)
        if beside is not None:
            beside(index, product[0, 0])
        product = scales[block] * product
        total = product if total is None else total + product
    return total


def coupler(base, total, dots, rows, rows_o, weights, other_t, coup):
    cuts = [total * index // dots for index in range(dots + 1)]
    taken = []

    def beside(_, value):
        if len(taken) == dots:
            return
        late = jnp.where(value == value, 0, 1)
        cut, share = cuts[len(taken)], cuts[len(taken) + 1] - cuts[len(taken)]
        start = jnp.minimum(base + cut + late, IFACE - share)
        taken.append(start)
        for v in range(share):
            slot = start + v
            coup[pl.ds(rows[slot], 1), :] = other_t[pl.ds(rows_o[slot], 1), :] * weights[slot]

    return beside


def inner_kernel(
    modes, prev, other, tables_in, *refs
):
    scalars, refs = refs[:5], refs[5:]
    partial_x, partial_p, coup, tables, flipped, blocks, other_t, sems = refs[:8]
    kinds, scales, rows, rows_o, weights, scalar_sems = refs[8:]
    fetched = fetch(scalars, (kinds, scales, rows, rows_o, weights), scalar_sems)
    loads = [
        pltpu.make_async_copy(
            tables_in.at[pl.ds(offset * NTYPE, NTYPE)],
            tables.at[pl.ds(offset * NTYPE, NTYPE)],
            sems.at[offset],
        )
        for offset in range(3)
    ]
    for offset in (1, 2, 0):
        loads[offset].start()
    for b in range(NBR):
        span = slice(b * BS, (b + 1) * BS)
        blocks[b] = jnp.concatenate([modes[:, span], prev[:, span]], axis=0).astype(BF16)
    for c in range(TILES):
        span = slice(c * LANES, (c + 1) * LANES)
        other_t[span, :PAIR] = other[:, span].astype(F32).T
    coup[...] = jnp.zeros_like(coup)
    for offset in (1, 2):
        loads[offset].wait()
        for index in range(NTYPE):
            flipped[(offset - 1) * NTYPE + index] = tables[offset * NTYPE + index].T
    loads[0].wait()
    for copy in fetched:
        copy.wait()
    steps = (NBR - 4) // INNER
    slots = IFACE // steps

    def step(index, carry):
        beside = coupler(index * slots, slots, 5 * INNER - 1, rows, rows_o, weights, other_t, coup)
        for u in range(INNER):
            b = 2 + index * INNER + u
            total = block_sum(b, b, blocks, tables, flipped, kinds, scales, beside)
            span = pl.ds(pl.multiple_of(b * BS, BS), BS)
            partial_x[:, span] = total[:MODES]
            partial_p[:, span] = total[MODES:]
        return carry

    lax.fori_loop(0, steps, step, 0)


def outer_kernel(
    modes, prev, near, far, partial_x, partial_p, coup, tables, flipped, kinds_in, scales_in,
    image_x, image_p, inverse_j, sums, ends, kinds, scales, scalar_sems,
):
    fetched = fetch((kinds_in, scales_in), (kinds, scales), scalar_sems)
    first = domain_index() * NBR
    even = is_even()
    for b in range(2):
        span = slice(b * BS, (b + 1) * BS)
        ends[b] = pick(even, far[:, span], near[:, span])
        ends[10 + b] = pick(even, near[:, span], far[:, span])
    for at, b in ENDS:
        span = slice(b * BS, (b + 1) * BS)
        ends[at] = jnp.concatenate([modes[:, span], prev[:, span]], axis=0).astype(BF16)

    for copy in fetched:
        copy.wait()

    def step(index, carry):
        for u in range(2):
            b = index * (NBR - 2) + u
            total = block_sum(b, 2 + index * 6 + u, ends, tables, flipped, kinds, scales)
            span = pl.ds(pl.multiple_of(b * BS, BS), BS)
            image_x[:, span] = total[:MODES]
            image_p[:, span] = total[MODES:]
        tiles = (TILES - 4 * BS // LANES) // 2
        for v in range(tiles):
            at = 2 * BS + (index * tiles + v) * LANES
            span = pl.ds(pl.multiple_of(at, LANES), LANES)
            carry = finish(span, partial_x, partial_p, carry)
        return carry

    def finish(span, source_x, source_p, carry):
        squares, crossed = carry
        coupled = coup[span, :].T
        value = source_x[:, span] + coupled[:MODES]
        image_x[:, span] = value
        image_p[:, span] = source_p[:, span] + coupled[MODES:PAIR]
        own = modes[:, span]
        return squares + own * own, crossed + own * value

    nothing = jnp.zeros((MODES, LANES), F32)
    carry = lax.fori_loop(0, 2, step, (nothing, nothing))
    on_diagonal = lax.broadcasted_iota(jnp.int32, (LANES, LANES), 0) == lax.broadcasted_iota(
        jnp.int32, (LANES, LANES), 1
    )
    lines = []
    for part in range(BS // LANES):
        span = slice(part * LANES, (part + 1) * LANES)
        lines.append(
            [
                jnp.sum(
                    jnp.where(on_diagonal, tables[kind, span, span].astype(F32), 0.0),
                    axis=0, keepdims=True,
                )
                for kind in range(NTYPE)
            ]
        )
    for c in range(TILES):
        b, part = divmod(c, BS // LANES)
        span = slice(c * LANES, (c + 1) * LANES)
        if not 2 <= b < NBR - 2:
            carry = finish(span, image_x, image_p, carry)
        kind = kinds[first + b]
        line = lines[part][0]
        for other_kind in range(1, NTYPE):
            line = jnp.where(kind == other_kind, lines[part][other_kind], line)
        inverse_j[:, span] = 1.0 / (scales[first + b] * line)
    squares, crossed = carry
    both = jnp.concatenate([squares, crossed, jnp.zeros((LANES - PAIR, LANES), F32)], axis=0)
    total = jnp.sum(both.T, axis=0, keepdims=True)
    sums[...] = jnp.broadcast_to(total, (ALL_DEV, LANES))


def residual_kernel(gathered, modes, image_x, inverse_j, residual, whole, to_near, to_far):
    total = jnp.sum(gathered[...], axis=0, keepdims=True)
    column = jnp.broadcast_to(total, (LANES, LANES)).T
    quotient = column[MODES:PAIR, :] / column[:MODES, :]
    for c in range(TILES):
        span = slice(c * LANES, (c + 1) * LANES)
        value = (image_x[:, span] - modes[:, span] * quotient) * inverse_j[:, span]
        residual[:, span] = value
        whole[:, span] = value.astype(BF16)
    even = is_even()
    head, tail = whole[:, :HALO], whole[:, ROWS - HALO :]
    to_near[...] = pick(even, tail, head)
    to_far[...] = pick(even, head, tail)


def inner_second_kernel(
    coupled, whole, other, tables, flipped, *refs
):
    del coupled
    scalars, refs = refs[:5], refs[5:]
    partial, coup, blocks, other_t, kinds, scales, rows, rows_o, weights, scalar_sems = refs
    fetched = fetch(scalars, (kinds, scales, rows, rows_o, weights), scalar_sems)
    for b in range(NBR):
        blocks[b, :MODES] = whole[:, b * BS : (b + 1) * BS]
    for c in range(TILES):
        span = slice(c * LANES, (c + 1) * LANES)
        other_t[span, :MODES] = other[:, span].astype(F32).T
    for copy in fetched:
        copy.wait()
    steps = (NBR - 4) // INNER
    slots = IFACE // steps

    def blocked(index, carry):
        beside = coupler(index * slots, slots, 5 * INNER - 1, rows, rows_o, weights, other_t, coup)
        for u in range(INNER):
            b = 2 + index * INNER + u
            total = block_sum(b, b, blocks, tables, flipped, kinds, scales, beside)
            partial[:, pl.ds(pl.multiple_of(b * BS, BS), BS)] = total[:MODES]
        return carry

    lax.fori_loop(0, steps, blocked, 0)


def outer_second_kernel(
    residual, whole, near, far, partial, coup, tables, flipped, kinds_in, scales_in,
    modes, prev, image_x, image_p, residual_out, packed, ends, image_e, gram, sem,
    kinds, scales, scalar_sems,
):
    fetched = fetch((kinds_in, scales_in), (kinds, scales), scalar_sems)
    even = is_even()
    stored = pltpu.make_async_copy(residual, residual_out, sem)
    stored.start()
    for b in range(2):
        span = slice(b * BS, (b + 1) * BS)
        ends[b, :MODES] = pick(even, far[:, span], near[:, span])
        ends[10 + b, :MODES] = pick(even, near[:, span], far[:, span])
    for at, b in ENDS:
        ends[at, :MODES] = whole[:, b * BS : (b + 1) * BS]
    gram[...] = jnp.zeros_like(gram)

    for copy in fetched:
        copy.wait()

    def blocked(index, carry):
        for u in range(2):
            b = index * (NBR - 2) + u
            total = block_sum(b, 2 + index * 6 + u, ends, tables, flipped, kinds, scales)
            at = (index * 2 + u) * BS
            image_e[:, pl.ds(pl.multiple_of(at, BS), BS)] = total[:MODES]
        return carry

    lax.fori_loop(0, 2, blocked, 0)

    def add(b, block_part):
        span = pl.ds(pl.multiple_of(b * 2 * BS, 2 * BS), 2 * BS)
        coupled = [
            coup[pl.ds(pl.multiple_of(b * 2 * BS + c * LANES, LANES), LANES), :].T[:MODES]
            for c in range(2 * BS // LANES)
        ]
        image = block_part + jnp.concatenate(coupled, axis=1)
        parts = [ref[:, span] for ref in (modes, residual, prev, image_x)]
        both = jnp.concatenate([*parts, image, image_p[:, span]], axis=0)
        high = both.astype(BF16)
        low = (both - high.astype(F32)).astype(BF16)
        gram[...] += lax.dot_general(
            jnp.concatenate([high, low], axis=0), high, (((1,), (1,)), ((), ())),
            preferred_element_type=F32,
        )

    def step(index, carry):
        for u in range(3):
            b = 1 + index * 3 + u
            add(b, partial[:, pl.ds(pl.multiple_of(b * 2 * BS, 2 * BS), 2 * BS)])
        return carry

    last = NBR // 2 - 1
    lax.fori_loop(0, last // 3, step, 0)
    add(0, image_e[:, : 2 * BS])
    add(last, image_e[:, 2 * BS :])
    n = 3 * MODES
    pad = LANES - n
    zero_r = jnp.zeros((pad, n), F32)
    zero_c = jnp.zeros((LANES, pad), F32)

    def square(top, lane):
        value = gram[top : top + n, lane : lane + n]
        return jnp.concatenate([jnp.concatenate([value, zero_r], axis=0), zero_c], axis=1)

    cross_b = square(2 * n, 0)
    gram_b = square(0, 0) + cross_b + cross_b.T
    cross_a = square(0, n) + square(2 * n, n)
    raw = cross_a + square(3 * n, 0).T
    gram_a = raw + raw.T
    row = lax.broadcasted_iota(jnp.int32, (LANES, LANES), 0)
    col = lax.broadcasted_iota(jnp.int32, (LANES, LANES), 1)
    diagonal = jnp.sum(jnp.where(row == col, gram_a, 0.0), axis=0, keepdims=True)
    merged = jnp.where(row >= col, gram_b, gram_a)
    packed[...] = jnp.where(row == n, jnp.broadcast_to(diagonal, (LANES, LANES)), merged)
    stored.wait()


def lower_inverse(gram, count):
    group = 4
    tiles = count // 8
    sub = lax.broadcasted_iota(jnp.int32, (8, LANES), 0)
    lane = lax.broadcasted_iota(jnp.int32, (8, LANES), 1)
    left = [gram[8 * t : 8 * t + 8, :] for t in range(tiles)]
    right = [jnp.where(lane == sub + 8 * t, 1.0, 0.0).astype(F32) for t in range(tiles)]

    def spread(first):
        return [
            {
                t: jnp.broadcast_to(left[t][:, first + m : first + m + 1], (8, LANES))
                for t in range(first // 8, tiles)
            }
            for m in range(group)
        ]

    ahead = spread(0)
    for start in range(0, count, group):
        now = ahead
        ahead = spread(start + group) if start + group < count else []
        for k in range(group):
            pivot = start + k
            tile, r = divmod(pivot, 8)
            root = lax.rsqrt(now[k][tile][r : r + 1, :])
            factor = {t: now[k][t] * root for t in range(tile, tiles)}
            factor[tile] = jnp.where(sub > r, factor[tile], 0.0)
            for first, columns in ((start, now), (start + group, ahead)):
                for m, column in enumerate(columns):
                    at = first + m
                    if at <= pivot:
                        continue
                    own = factor[at // 8][at % 8 : at % 8 + 1, :]
                    for t in column:
                        column[t] = column[t] - factor[t] * own
            line_l = left[tile][r : r + 1, :] * root
            line_r = right[tile][r : r + 1, :] * root
            for t in range(tile, tiles):
                left[t] = left[t] - factor[t] * line_l
                right[t] = right[t] - factor[t] * line_r
            right[tile] = jnp.where(sub == r, line_r, right[tile])
    return right


def final_kernel(packed, modes, residual_in, prev, basis, projected, result, residual, sems):
    n = 3 * MODES
    load = pltpu.make_async_copy(residual_in, residual, sems.at[ROWS // WIDTH])
    load.start()
    row = lax.broadcasted_iota(jnp.int32, (LANES, LANES), 0)
    col = lax.broadcasted_iota(jnp.int32, (LANES, LANES), 1)
    merged = packed[...]
    flipped = merged.T
    inside = (row < n) & (col < n)
    ndof = jnp.float32(2.0 * 64 * ROWS)
    gram_b = jnp.where(inside, jnp.where(row >= col, merged, flipped) / ndof, 0.0)
    diagonal = jnp.broadcast_to(merged[n : n + 1, :], (LANES, LANES))
    gram_a = jnp.where(row < col, merged, flipped)
    gram_a = jnp.where(row == col, diagonal, gram_a) / (2.0 * ndof)
    gram_a = jnp.where(inside, gram_a, 0.0)
    factors = jnp.concatenate(lower_inverse(gram_b, n), axis=0)
    square = factors[:, :n]
    high = square.astype(BF16)
    low = (square - high.astype(F32)).astype(BF16)
    top = jnp.concatenate([high, high], axis=1)
    dims = (((1,), (0,)), ((), ()))
    load.wait()
    stores = []
    for index in range(ROWS // WIDTH):
        span = pl.ds(index * WIDTH, WIDTH)
        part = jnp.concatenate([modes[:, span], residual[:, span], prev[:, span]], axis=0)
        part_h = part.astype(BF16)
        part_l = (part - part_h.astype(F32)).astype(BF16)
        stacked = jnp.concatenate([part_h, part_l], axis=0)
        result[:, span] = lax.dot_general(
            top, stacked, dims, preferred_element_type=F32
        ) + lax.dot_general(low, part_h, dims, preferred_element_type=F32)
        store = pltpu.make_async_copy(
            result.at[:, span], basis.at[:, span], sems.at[index]
        )
        store.start()
        stores.append(store)
    half = lax.dot_general(
        factors, gram_a, (((1,), (0,)), ((), ())),
        precision=lax.Precision.HIGHEST, preferred_element_type=F32,
    )
    whole = lax.dot_general(
        half, factors, (((1,), (1,)), ((), ())),
        precision=lax.Precision.HIGHEST, preferred_element_type=F32,
    )
    projected[...] = whole
    for store in stores:
        store.wait()


def shards(modes, previous, kinds, scales, tables, wet_rows, wet_counts, coupling):
    modes = modes[0]
    prev = previous[0]
    kinds = kinds[0].reshape(3 * NBLK)
    scales = scales[0].reshape(3 * NBLK)
    tables = tables[0].reshape(3 * NTYPE, BS, BS)
    rows = wet_rows[0]
    modes, prev, whole, to_near, to_far, weights, rows = rounded_parts(
        modes, prev, coupling, rows, wet_counts
    )
    weights = weights.reshape(IFACE)
    rows_o = swap_field(rows).reshape(IFACE)
    rows = rows.reshape(IFACE)
    other = swap_field(whole)
    near = swap_pairs(to_near, 0)
    far = swap_pairs(to_far, 1)
    coupling_args = (rows, rows_o, weights)
    plane = shape(MODES, ROWS)
    rows_by_lanes = shape(ROWS, LANES)
    end = shape(PAIR, HALO)
    partial_x, partial_p, coup, tables, flipped = pl.pallas_call(
        inner_kernel,
        out_shape=(
            plane, plane, rows_by_lanes,
            shape(3 * NTYPE, BS, BS, kind=BF16), shape(2 * NTYPE, BS, BS, kind=BF16),
        ),
        in_specs=[VMEM] * 3 + [HBM] + [VMEM] * 5,
        out_specs=[VMEM] * 5,
        scratch_shapes=[
            pltpu.VMEM((NBR, PAIR, BS), BF16),
            pltpu.VMEM((ROWS, LANES), F32),
            pltpu.SemaphoreType.DMA((3,)),
            *scalar_scratch(True),
        ],
        compiler_params=params(10),
        name="inner",
    )(modes, prev, other, in_hbm(tables), kinds, scales, *coupling_args)
    image_x, image_p, inverse_j, sums = pl.pallas_call(
        outer_kernel,
        out_shape=(plane, plane, shape(1, ROWS), shape(ALL_DEV, LANES)),
        in_specs=[VMEM] * 11,
        out_specs=[VMEM] * 4,
        scratch_shapes=[pltpu.VMEM((12, PAIR, BS), BF16), *scalar_scratch(False)],
        compiler_params=params(6),
        name="outer",
    )(modes, prev, near, far, partial_x, partial_p, coup, tables, flipped, kinds, scales)
    gathered = exchange(sums)
    end = shape(MODES, HALO, kind=BF16)
    residual, whole, to_near, to_far = pl.pallas_call(
        residual_kernel,
        out_shape=(plane, shape(MODES, ROWS, kind=BF16), end, end),
        in_specs=[VMEM] * 4,
        out_specs=[VMEM] * 4,
        compiler_params=params(6),
        name="residual",
    )(gathered, modes, image_x, inverse_j)
    other = swap_field(whole)
    near = swap_pairs(to_near, 0)
    far = swap_pairs(to_far, 1)
    partial, coup = pl.pallas_call(
        inner_second_kernel,
        out_shape=(plane, rows_by_lanes),
        in_specs=[VMEM] * 10,
        out_specs=[VMEM] * 2,
        input_output_aliases={0: 1},
        scratch_shapes=[
            pltpu.VMEM((NBR, SINGLE, BS), BF16),
            pltpu.VMEM((ROWS, LANES), F32),
            *scalar_scratch(True),
        ],
        compiler_params=params(10),
        name="inner_second",
    )(coup, whole, other, tables, flipped, kinds, scales, *coupling_args)
    residual, packed = pl.pallas_call(
        outer_second_kernel,
        out_shape=(pltpu.HBM((MODES, ROWS), F32), shape(LANES, LANES)),
        in_specs=[VMEM] * 14,
        out_specs=[HBM, VMEM],
        scratch_shapes=[
            pltpu.VMEM((12, SINGLE, BS), BF16),
            pltpu.VMEM((MODES, 4 * BS), F32),
            pltpu.VMEM((12 * MODES, 6 * MODES), F32),
            pltpu.SemaphoreType.DMA(()),
            *scalar_scratch(False),
        ],
        compiler_params=params(10),
        name="outer_second",
    )(
        residual, whole, near, far, partial, coup, tables, flipped, kinds, scales,
        modes, prev, image_x, image_p,
    )
    part = jnp.sum(exchange(packed), axis=0, keepdims=True)
    packed = exchange(jnp.broadcast_to(part, (ALL_DEV, LANES)))
    n = 3 * MODES
    basis, projected = pl.pallas_call(
        final_kernel,
        out_shape=(pltpu.HBM((n, ROWS), F32), shape(n, n)),
        in_specs=[VMEM, VMEM, HBM, VMEM],
        out_specs=[HBM, VMEM],
        scratch_shapes=[
            pltpu.VMEM((n, ROWS), F32),
            pltpu.VMEM((MODES, ROWS), F32),
            pltpu.SemaphoreType.DMA((ROWS // WIDTH + 1,)),
        ],
        compiler_params=params(14),
        name="final",
    )(packed, modes, in_hbm(residual), prev)
    return (basis[None], projected)


def solution(mesh):
    finer = Mesh(
        mesh.devices.reshape(mesh.shape["field"], 4, 4, 4), ("field", "dom_0", "dom_1", "dom_2")
    )
    placed = (
        P("field", None, DOM),
        P("field", None, DOM),
        P("field", None, None),
        P("field", None, None),
        P("field", None, None, None, None),
        P("field", DOM),
        P(DOM),
        P(DOM),
    )
    return jax.shard_map(
        shards, mesh=finer, in_specs=placed, out_specs=(P("field", None, DOM), P()), check_vma=False
    )
```

```python
import jax
import jax.numpy as jnp
from jax import lax
from jax.experimental import pallas as pl
from jax.experimental.pallas import tpu as pltpu
from jax.sharding import Mesh
from jax.sharding import PartitionSpec as P


BS = 512
NTYPE = 4
NBR = 16
NBLK = 1024
ROWS = NBR * BS
HALO = 2 * BS
MODES = 40
IFACE = 3072
LANES = 128
TILES = ROWS // LANES
DOM = ("dom_0", "dom_1", "dom_2")
FIELD_DOM = ("field", "dom_0", "dom_1", "dom_2")
ALL_DEV = 128
F32 = jnp.float32
BF16 = jnp.bfloat16

VMEM = pl.BlockSpec(memory_space=pltpu.VMEM)
SMEM = pl.BlockSpec(memory_space=pltpu.SMEM)
HBM = pl.BlockSpec(memory_space=pltpu.HBM)
PAIR = 2 * MODES
SINGLE = 48
INNER = 12
ENDS = ((2, 0), (3, 1), (4, 2), (5, 3), (6, 12), (7, 13), (8, 14), (9, 15))
WIDTH = 1024
EARLY = 16

OPS = ((0, 0, 0, 0), (1, -1, -1, 0), (2, -2, -2, 0), (1, 1, 0, 1), (2, 2, 0, 1))


def params(mib):
    return pltpu.CompilerParams(vmem_limit_bytes=mib << 20)


def shape(*dims, kind=F32):
    return jax.ShapeDtypeStruct(dims, kind)


def domain_index():
    return (lax.axis_index(DOM[0]) * 4 + lax.axis_index(DOM[1])) * 4 + lax.axis_index(DOM[2])


def in_hbm(value):
    return pltpu.with_memory_space_constraint(value, pltpu.HBM)


def swap_field(value):
    return lax.ppermute(value, "field", [(0, 1), (1, 0)])


def is_even():
    return lax.rem(lax.axis_index(DOM[2]), 2) == 0


def pick(condition, one, two):
    return jnp.where(condition, one, two)


def swap_pairs(value, first):
    pairs = [(i, i + 1) for i in range(first, 63, 2)]
    return lax.ppermute(value, DOM, pairs + [(j, i) for i, j in pairs])


def exchange(rows):
    return lax.all_to_all(rows, FIELD_DOM, 0, 0, tiled=True)


def round_kernel(
    modes, prev, coupling, rows, counts,
    modes_v, prev_v, whole, to_near, to_far, weights, rows_v, sems,
):
    pairs = ((modes, modes_v), (prev, prev_v), (coupling, weights), (rows, rows_v))
    loads = [
        pltpu.make_async_copy(source, target, sems.at[index])
        for index, (source, target) in enumerate(pairs)
    ]
    for load in loads:
        load.start()
    slot = lax.broadcasted_iota(jnp.int32, weights.shape, 0) * LANES + lax.broadcasted_iota(
        jnp.int32, weights.shape, 1
    )
    for load in loads:
        load.wait()
    weights[...] = jnp.where(slot < counts[0], weights[...], 0.0)
    rounded = jnp.concatenate([modes_v[...], prev_v[...]], axis=0).astype(BF16)
    whole[...] = rounded
    even = is_even()
    head, tail = rounded[:, :HALO], rounded[:, ROWS - HALO :]
    to_near[...] = pick(even, tail, head)
    to_far[...] = pick(even, head, tail)


def rounded_parts(modes, prev, coupling, rows, counts):
    plane = shape(MODES, ROWS)
    end = shape(PAIR, HALO, kind=BF16)
    slots = shape(IFACE // LANES, LANES)
    return pl.pallas_call(
        round_kernel,
        out_shape=(plane, plane, shape(PAIR, ROWS, kind=BF16), end, end, slots,
                   shape(IFACE // LANES, LANES, kind=jnp.int32)),
        in_specs=[HBM] * 4 + [SMEM],
        out_specs=[VMEM] * 7,
        scratch_shapes=[pltpu.SemaphoreType.DMA((4,))],
        compiler_params=params(12),
        name="rounded",
    )(
        *map(in_hbm, (modes, prev, coupling.reshape(slots.shape), rows.reshape(slots.shape))),
        counts,
    )


def fetch(sources, targets, sems):
    copies = [
        pltpu.make_async_copy(source, target, sems.at[index])
        for index, (source, target) in enumerate(zip(sources, targets))
    ]
    for copy in copies:
        copy.start()
    return copies


def scalar_scratch(coupled):
    kinds = [jnp.int32, F32] + [jnp.int32, jnp.int32, F32] * coupled
    return [pltpu.SMEM((IFACE,), kind) for kind in kinds] + [
        pltpu.SemaphoreType.DMA((len(kinds),))
    ]


def block_sum(b, at, blocks, tables, flipped, kinds, scales, beside=None):
    first = domain_index() * NBR
    total = None
    for index, (offset, shift, owner, flip) in enumerate(OPS):
        block = offset * NBLK + jnp.maximum(first + b + owner, 0)
        kind = kinds[block]
        if flip:
            table = flipped[(offset - 1) * NTYPE + kind]
        else:
            table = tables[offset * NTYPE + kind]
        product = jnp.dot(blocks[at + shift], table, preferred_element_type=F32)
        if beside is not None:
            beside(index, product[0, 0])
        product = scales[block] * product
        total = product if total is None else total + product
    return total


def coupler(base, total, dots, rows, rows_o, weights, other_t, coup):
    cuts = [total * index // dots for index in range(dots + 1)]
    taken = []

    def beside(_, value):
        if len(taken) == dots:
            return
        late = jnp.where(value == value, 0, 1)
        cut, share = cuts[len(taken)], cuts[len(taken) + 1] - cuts[len(taken)]
        start = jnp.minimum(base + cut + late, IFACE - share)
        taken.append(start)
        for v in range(share):
            slot = start + v
            coup[pl.ds(rows[slot], 1), :] = other_t[pl.ds(rows_o[slot], 1), :] * weights[slot]

    return beside


def inner_kernel(
    modes, prev, other, tables_in, *refs
):
    scalars, refs = refs[:5], refs[5:]
    partial_x, partial_p, coup, tables, flipped, blocks, other_t, sems = refs[:8]
    kinds, scales, rows, rows_o, weights, scalar_sems = refs[8:]
    fetched = fetch(scalars, (kinds, scales, rows, rows_o, weights), scalar_sems)
    loads = [
        pltpu.make_async_copy(
            tables_in.at[pl.ds(offset * NTYPE, NTYPE)],
            tables.at[pl.ds(offset * NTYPE, NTYPE)],
            sems.at[offset],
        )
        for offset in range(3)
    ]
    for offset in (1, 2, 0):
        loads[offset].start()
    for b in range(NBR):
        span = slice(b * BS, (b + 1) * BS)
        blocks[b] = jnp.concatenate([modes[:, span], prev[:, span]], axis=0).astype(BF16)
    for c in range(TILES):
        span = slice(c * LANES, (c + 1) * LANES)
        other_t[span, :PAIR] = other[:, span].astype(F32).T
    coup[...] = jnp.zeros_like(coup)
    for offset in (1, 2):
        loads[offset].wait()
        for index in range(NTYPE):
            flipped[(offset - 1) * NTYPE + index] = tables[offset * NTYPE + index].T
    loads[0].wait()
    for copy in fetched:
        copy.wait()
    steps = (NBR - 4) // INNER
    slots = IFACE // steps

    def step(index, carry):
        beside = coupler(index * slots, slots, 5 * INNER - 1, rows, rows_o, weights, other_t, coup)
        for u in range(INNER):
            b = 2 + index * INNER + u
            total = block_sum(b, b, blocks, tables, flipped, kinds, scales, beside)
            span = pl.ds(pl.multiple_of(b * BS, BS), BS)
            partial_x[:, span] = total[:MODES]
            partial_p[:, span] = total[MODES:]
        return carry

    lax.fori_loop(0, steps, step, 0)


def outer_kernel(
    modes, prev, near, far, partial_x, partial_p, coup, tables, flipped, kinds_in, scales_in,
    image_x, image_p, inverse_j, sums, ends, kinds, scales, scalar_sems,
):
    fetched = fetch((kinds_in, scales_in), (kinds, scales), scalar_sems)
    first = domain_index() * NBR
    even = is_even()
    for b in range(2):
        span = slice(b * BS, (b + 1) * BS)
        ends[b] = pick(even, far[:, span], near[:, span])
        ends[10 + b] = pick(even, near[:, span], far[:, span])
    for at, b in ENDS:
        span = slice(b * BS, (b + 1) * BS)
        ends[at] = jnp.concatenate([modes[:, span], prev[:, span]], axis=0).astype(BF16)

    def finish(span, source_x, source_p, carry):
        squares, crossed = carry
        coupled = coup[span, :].T
        value = source_x[:, span] + coupled[:MODES]
        image_x[:, span] = value
        image_p[:, span] = source_p[:, span] + coupled[MODES:PAIR]
        own = modes[:, span]
        return squares + own * own, crossed + own * value

    on_diagonal = lax.broadcasted_iota(jnp.int32, (LANES, LANES), 0) == lax.broadcasted_iota(
        jnp.int32, (LANES, LANES), 1
    )
    lines = []
    for part in range(BS // LANES):
        span = slice(part * LANES, (part + 1) * LANES)
        lines.append(
            [
                jnp.sum(
                    jnp.where(on_diagonal, tables[kind, span, span].astype(F32), 0.0),
                    axis=0, keepdims=True,
                )
                for kind in range(NTYPE)
            ]
        )
    carry = (jnp.zeros((MODES, LANES), F32),) * 2
    for c in range(EARLY):
        carry = finish(slice(2 * BS + c * LANES, 2 * BS + (c + 1) * LANES), partial_x, partial_p, carry)
    for copy in fetched:
        copy.wait()

    def step(index, carry):
        for u in range(2):
            b = index * (NBR - 2) + u
            total = block_sum(b, 2 + index * 6 + u, ends, tables, flipped, kinds, scales)
            span = pl.ds(pl.multiple_of(b * BS, BS), BS)
            image_x[:, span] = total[:MODES]
            image_p[:, span] = total[MODES:]
        tiles = (TILES - 4 * BS // LANES - EARLY) // 2
        for v in range(tiles):
            at = 2 * BS + (EARLY + index * tiles + v) * LANES
            span = pl.ds(pl.multiple_of(at, LANES), LANES)
            carry = finish(span, partial_x, partial_p, carry)
        return carry

    carry = lax.fori_loop(0, 2, step, carry)
    for c in range(TILES):
        b, part = divmod(c, BS // LANES)
        span = slice(c * LANES, (c + 1) * LANES)
        if not 2 <= b < NBR - 2:
            carry = finish(span, image_x, image_p, carry)
        kind = kinds[first + b]
        line = lines[part][0]
        for other_kind in range(1, NTYPE):
            line = jnp.where(kind == other_kind, lines[part][other_kind], line)
        inverse_j[:, span] = 1.0 / (scales[first + b] * line)
    squares, crossed = carry
    both = jnp.concatenate([squares, crossed, jnp.zeros((LANES - PAIR, LANES), F32)], axis=0)
    total = jnp.sum(both.T, axis=0, keepdims=True)
    sums[...] = jnp.broadcast_to(total, (ALL_DEV, LANES))


def residual_kernel(gathered, modes, image_x, inverse_j, residual, whole, to_near, to_far):
    total = jnp.sum(gathered[...], axis=0, keepdims=True)
    column = jnp.broadcast_to(total, (LANES, LANES)).T
    quotient = column[MODES:PAIR, :] / column[:MODES, :]
    for c in range(TILES):
        span = slice(c * LANES, (c + 1) * LANES)
        value = (image_x[:, span] - modes[:, span] * quotient) * inverse_j[:, span]
        residual[:, span] = value
        whole[:, span] = value.astype(BF16)
    even = is_even()
    head, tail = whole[:, :HALO], whole[:, ROWS - HALO :]
    to_near[...] = pick(even, tail, head)
    to_far[...] = pick(even, head, tail)


def inner_second_kernel(
    coupled, whole, other, tables, flipped, *refs
):
    del coupled
    scalars, refs = refs[:5], refs[5:]
    partial, coup, blocks, other_t, kinds, scales, rows, rows_o, weights, scalar_sems = refs
    fetched = fetch(scalars, (kinds, scales, rows, rows_o, weights), scalar_sems)
    for b in range(NBR):
        blocks[b, :MODES] = whole[:, b * BS : (b + 1) * BS]
    for c in range(TILES):
        span = slice(c * LANES, (c + 1) * LANES)
        other_t[span, :MODES] = other[:, span].astype(F32).T
    for copy in fetched:
        copy.wait()
    steps = (NBR - 4) // INNER
    slots = IFACE // steps

    def blocked(index, carry):
        beside = coupler(index * slots, slots, 5 * INNER - 1, rows, rows_o, weights, other_t, coup)
        for u in range(INNER):
            b = 2 + index * INNER + u
            total = block_sum(b, b, blocks, tables, flipped, kinds, scales, beside)
            partial[:, pl.ds(pl.multiple_of(b * BS, BS), BS)] = total[:MODES]
        return carry

    lax.fori_loop(0, steps, blocked, 0)


def outer_second_kernel(
    residual, whole, near, far, partial, coup, tables, flipped, kinds_in, scales_in,
    modes, prev, image_x, image_p, residual_out, packed, ends, image_e, gram, sem,
    kinds, scales, scalar_sems,
):
    fetched = fetch((kinds_in, scales_in), (kinds, scales), scalar_sems)
    even = is_even()
    stored = pltpu.make_async_copy(residual, residual_out, sem)
    stored.start()
    for b in range(2):
        span = slice(b * BS, (b + 1) * BS)
        ends[b, :MODES] = pick(even, far[:, span], near[:, span])
        ends[10 + b, :MODES] = pick(even, near[:, span], far[:, span])
    for at, b in ENDS:
        ends[at, :MODES] = whole[:, b * BS : (b + 1) * BS]
    gram[...] = jnp.zeros_like(gram)

    def add(b, block_part):
        span = pl.ds(pl.multiple_of(b * 2 * BS, 2 * BS), 2 * BS)
        coupled = [
            coup[pl.ds(pl.multiple_of(b * 2 * BS + c * LANES, LANES), LANES), :].T[:MODES]
            for c in range(2 * BS // LANES)
        ]
        image = block_part + jnp.concatenate(coupled, axis=1)
        parts = [ref[:, span] for ref in (modes, residual, prev, image_x)]
        both = jnp.concatenate([*parts, image, image_p[:, span]], axis=0)
        high = both.astype(BF16)
        low = (both - high.astype(F32)).astype(BF16)
        gram[...] += lax.dot_general(
            jnp.concatenate([high, low], axis=0), high, (((1,), (1,)), ((), ())),
            preferred_element_type=F32,
        )

    def step(index, carry):
        for u in range(3):
            b = 1 + index * 3 + u
            add(b, partial[:, pl.ds(pl.multiple_of(b * 2 * BS, 2 * BS), 2 * BS)])
        return carry

    last = NBR // 2 - 1
    lax.fori_loop(0, last // 3, step, 0)
    for copy in fetched:
        copy.wait()

    def blocked(index, carry):
        for u in range(2):
            b = index * (NBR - 2) + u
            total = block_sum(b, 2 + index * 6 + u, ends, tables, flipped, kinds, scales)
            at = (index * 2 + u) * BS
            image_e[:, pl.ds(pl.multiple_of(at, BS), BS)] = total[:MODES]
        return carry

    lax.fori_loop(0, 2, blocked, 0)
    add(0, image_e[:, : 2 * BS])
    add(last, image_e[:, 2 * BS :])
    n = 3 * MODES
    pad = LANES - n
    zero_r = jnp.zeros((pad, n), F32)
    zero_c = jnp.zeros((LANES, pad), F32)

    def square(top, lane):
        value = gram[top : top + n, lane : lane + n]
        return jnp.concatenate([jnp.concatenate([value, zero_r], axis=0), zero_c], axis=1)

    cross_b = square(2 * n, 0)
    gram_b = square(0, 0) + cross_b + cross_b.T
    cross_a = square(0, n) + square(2 * n, n)
    raw = cross_a + square(3 * n, 0).T
    gram_a = raw + raw.T
    row = lax.broadcasted_iota(jnp.int32, (LANES, LANES), 0)
    col = lax.broadcasted_iota(jnp.int32, (LANES, LANES), 1)
    diagonal = jnp.sum(jnp.where(row == col, gram_a, 0.0), axis=0, keepdims=True)
    merged = jnp.where(row >= col, gram_b, gram_a)
    packed[...] = jnp.where(row == n, jnp.broadcast_to(diagonal, (LANES, LANES)), merged)
    stored.wait()


def lower_inverse(gram, count):
    group = 4
    tiles = count // 8
    sub = lax.broadcasted_iota(jnp.int32, (8, LANES), 0)
    lane = lax.broadcasted_iota(jnp.int32, (8, LANES), 1)
    left = [gram[8 * t : 8 * t + 8, :] for t in range(tiles)]
    right = [jnp.where(lane == sub + 8 * t, 1.0, 0.0).astype(F32) for t in range(tiles)]

    def spread(first):
        return [
            {
                t: jnp.broadcast_to(left[t][:, first + m : first + m + 1], (8, LANES))
                for t in range(first // 8, tiles)
            }
            for m in range(group)
        ]

    ahead = spread(0)
    for start in range(0, count, group):
        now = ahead
        ahead = spread(start + group) if start + group < count else []
        for k in range(group):
            pivot = start + k
            tile, r = divmod(pivot, 8)
            root = lax.rsqrt(now[k][tile][r : r + 1, :])
            factor = {t: now[k][t] * root for t in range(tile, tiles)}
            factor[tile] = jnp.where(sub > r, factor[tile], 0.0)
            for first, columns in ((start, now), (start + group, ahead)):
                for m, column in enumerate(columns):
                    at = first + m
                    if at <= pivot:
                        continue
                    own = factor[at // 8][at % 8 : at % 8 + 1, :]
                    for t in column:
                        column[t] = column[t] - factor[t] * own
            line_l = left[tile][r : r + 1, :] * root
            line_r = right[tile][r : r + 1, :] * root
            for t in range(tile, tiles):
                left[t] = left[t] - factor[t] * line_l
                right[t] = right[t] - factor[t] * line_r
            right[tile] = jnp.where(sub == r, line_r, right[tile])
    return right


def final_kernel(packed, modes, residual_in, prev, basis, projected, result, residual, sems):
    n = 3 * MODES
    load = pltpu.make_async_copy(residual_in, residual, sems.at[ROWS // WIDTH])
    load.start()
    row = lax.broadcasted_iota(jnp.int32, (LANES, LANES), 0)
    col = lax.broadcasted_iota(jnp.int32, (LANES, LANES), 1)
    merged = packed[...]
    flipped = merged.T
    inside = (row < n) & (col < n)
    ndof = jnp.float32(2.0 * 64 * ROWS)
    gram_b = jnp.where(inside, jnp.where(row >= col, merged, flipped) / ndof, 0.0)
    diagonal = jnp.broadcast_to(merged[n : n + 1, :], (LANES, LANES))
    gram_a = jnp.where(row < col, merged, flipped)
    gram_a = jnp.where(row == col, diagonal, gram_a) / (2.0 * ndof)
    gram_a = jnp.where(inside, gram_a, 0.0)
    factors = jnp.concatenate(lower_inverse(gram_b, n), axis=0)
    square = factors[:, :n]
    high = square.astype(BF16)
    low = (square - high.astype(F32)).astype(BF16)
    top = jnp.concatenate([high, high], axis=1)
    dims = (((1,), (0,)), ((), ()))
    load.wait()
    stores = []
    for index in range(ROWS // WIDTH):
        span = pl.ds(index * WIDTH, WIDTH)
        part = jnp.concatenate([modes[:, span], residual[:, span], prev[:, span]], axis=0)
        part_h = part.astype(BF16)
        part_l = (part - part_h.astype(F32)).astype(BF16)
        stacked = jnp.concatenate([part_h, part_l], axis=0)
        result[:, span] = lax.dot_general(
            top, stacked, dims, preferred_element_type=F32
        ) + lax.dot_general(low, part_h, dims, preferred_element_type=F32)
        store = pltpu.make_async_copy(
            result.at[:, span], basis.at[:, span], sems.at[index]
        )
        store.start()
        stores.append(store)
    half = lax.dot_general(
        factors, gram_a, (((1,), (0,)), ((), ())),
        precision=lax.Precision.HIGHEST, preferred_element_type=F32,
    )
    whole = lax.dot_general(
        half, factors, (((1,), (1,)), ((), ())),
        precision=lax.Precision.HIGHEST, preferred_element_type=F32,
    )
    projected[...] = whole
    for store in stores:
        store.wait()


def shards(modes, previous, kinds, scales, tables, wet_rows, wet_counts, coupling):
    modes = modes[0]
    prev = previous[0]
    kinds = kinds[0].reshape(3 * NBLK)
    scales = scales[0].reshape(3 * NBLK)
    tables = tables[0].reshape(3 * NTYPE, BS, BS)
    rows = wet_rows[0]
    modes, prev, whole, to_near, to_far, weights, rows = rounded_parts(
        modes, prev, coupling, rows, wet_counts
    )
    weights = weights.reshape(IFACE)
    rows_o = swap_field(rows).reshape(IFACE)
    rows = rows.reshape(IFACE)
    other = swap_field(whole)
    near = swap_pairs(to_near, 0)
    far = swap_pairs(to_far, 1)
    coupling_args = (rows, rows_o, weights)
    plane = shape(MODES, ROWS)
    rows_by_lanes = shape(ROWS, LANES)
    end = shape(PAIR, HALO)
    partial_x, partial_p, coup, tables, flipped = pl.pallas_call(
        inner_kernel,
        out_shape=(
            plane, plane, rows_by_lanes,
            shape(3 * NTYPE, BS, BS, kind=BF16), shape(2 * NTYPE, BS, BS, kind=BF16),
        ),
        in_specs=[VMEM] * 3 + [HBM] + [VMEM] * 5,
        out_specs=[VMEM] * 5,
        scratch_shapes=[
            pltpu.VMEM((NBR, PAIR, BS), BF16),
            pltpu.VMEM((ROWS, LANES), F32),
            pltpu.SemaphoreType.DMA((3,)),
            *scalar_scratch(True),
        ],
        compiler_params=params(10),
        name="inner",
    )(modes, prev, other, in_hbm(tables), kinds, scales, *coupling_args)
    image_x, image_p, inverse_j, sums = pl.pallas_call(
        outer_kernel,
        out_shape=(plane, plane, shape(1, ROWS), shape(ALL_DEV, LANES)),
        in_specs=[VMEM] * 11,
        out_specs=[VMEM] * 4,
        scratch_shapes=[pltpu.VMEM((12, PAIR, BS), BF16), *scalar_scratch(False)],
        compiler_params=params(6),
        name="outer",
    )(modes, prev, near, far, partial_x, partial_p, coup, tables, flipped, kinds, scales)
    gathered = exchange(sums)
    end = shape(MODES, HALO, kind=BF16)
    residual, whole, to_near, to_far = pl.pallas_call(
        residual_kernel,
        out_shape=(plane, shape(MODES, ROWS, kind=BF16), end, end),
        in_specs=[VMEM] * 4,
        out_specs=[VMEM] * 4,
        compiler_params=params(6),
        name="residual",
    )(gathered, modes, image_x, inverse_j)
    other = swap_field(whole)
    near = swap_pairs(to_near, 0)
    far = swap_pairs(to_far, 1)
    partial, coup = pl.pallas_call(
        inner_second_kernel,
        out_shape=(plane, rows_by_lanes),
        in_specs=[VMEM] * 10,
        out_specs=[VMEM] * 2,
        input_output_aliases={0: 1},
        scratch_shapes=[
            pltpu.VMEM((NBR, SINGLE, BS), BF16),
            pltpu.VMEM((ROWS, LANES), F32),
            *scalar_scratch(True),
        ],
        compiler_params=params(10),
        name="inner_second",
    )(coup, whole, other, tables, flipped, kinds, scales, *coupling_args)
    residual, packed = pl.pallas_call(
        outer_second_kernel,
        out_shape=(pltpu.HBM((MODES, ROWS), F32), shape(LANES, LANES)),
        in_specs=[VMEM] * 14,
        out_specs=[HBM, VMEM],
        scratch_shapes=[
            pltpu.VMEM((12, SINGLE, BS), BF16),
            pltpu.VMEM((MODES, 4 * BS), F32),
            pltpu.VMEM((12 * MODES, 6 * MODES), F32),
            pltpu.SemaphoreType.DMA(()),
            *scalar_scratch(False),
        ],
        compiler_params=params(10),
        name="outer_second",
    )(
        residual, whole, near, far, partial, coup, tables, flipped, kinds, scales,
        modes, prev, image_x, image_p,
    )
    part = jnp.sum(exchange(packed), axis=0, keepdims=True)
    packed = exchange(jnp.broadcast_to(part, (ALL_DEV, LANES)))
    n = 3 * MODES
    basis, projected = pl.pallas_call(
        final_kernel,
        out_shape=(pltpu.HBM((n, ROWS), F32), shape(n, n)),
        in_specs=[VMEM, VMEM, HBM, VMEM],
        out_specs=[HBM, VMEM],
        scratch_shapes=[
            pltpu.VMEM((n, ROWS), F32),
            pltpu.VMEM((MODES, ROWS), F32),
            pltpu.SemaphoreType.DMA((ROWS // WIDTH + 1,)),
        ],
        compiler_params=params(14),
        name="final",
    )(packed, modes, in_hbm(residual), prev)
    return (basis[None], projected)


def solution(mesh):
    finer = Mesh(
        mesh.devices.reshape(mesh.shape["field"], 4, 4, 4), ("field", "dom_0", "dom_1", "dom_2")
    )
    placed = (
        P("field", None, DOM),
        P("field", None, DOM),
        P("field", None, None),
        P("field", None, None),
        P("field", None, None, None, None),
        P("field", DOM),
        P(DOM),
        P(DOM),
    )
    return jax.shard_map(
        shards, mesh=finer, in_specs=placed, out_specs=(P("field", None, DOM), P()), check_vma=False
    )
```
